512 devices in a mesh: groups: 2 (over y), beam: 128 (over z, x), mp: 2 (over core).
Axes of the slice: x: 4, y: 2, z: 32, core: 2. Of those that a mesh axis runs over, the one named last changes fastest.
The devices are a block of a 4x8x32 slice.
Arguments:
- states: float32 [1024, 8, 128, 128], P(('groups', 'beam'), 'mp'), parts along dimension 0, may hold values from -4 to 4
- parent_beam: int32 [1024], P(('groups', 'beam')), parts along dimension 0, may hold values from 0 to 7, as said below
- next_token: int32 [1024], P(('groups', 'beam')), parts along dimension 0, may hold values from 0 to 16383
- proj_table: bfloat16 [16384, 8, 640], P('beam', 'mp'), may hold values from -6 to 6
- gate_table: bfloat16 [16384, 3, 8], P('beam', None, 'mp'), may hold values from -6 to 6
- gain: float32 [8, 128], P('mp'), may hold values from 0.1 to 1.9
Outputs:
- readout: bfloat16 [1024, 8, 128], P(('groups', 'beam'), 'mp'), parts along dimension 0
- new_states: float32 [1024, 8, 128, 128], P(('groups', 'beam'), 'mp'), parts along dimension 0
The draws below stay inside these ranges and needn't reach their ends.
There are 2 independent parts, one for each index of `groups`. The reference program is written for one: setup_inputs(seed, part) draws one part's arguments, and reference() takes and returns one part's arrays. A program takes and returns all parts, laid end to end along the dimension named above; an argument that names none is the same for every part. Nothing has to cross between parts.
Inputs may be any that keep to these rules, and one draw needn't show every extreme that they name: The parent of hypothesis h = b * 64 + u is parent_beam[h] * 64 + u. In each aligned block of 4 hypotheses at most 2 take their parent from any one beam other than their own beam, and every block has a beam that supplies exactly 2.
All inputs are finite; a program needn't handle non-finite values.
Results may differ from the reference program's by a relative error of at most 0.001.
Values may be sent and summed in bfloat16 or wider, within the bound.
A program may use at most 64 MiB of HBM per device.

```python
import math
import jax
import jax.numpy as jnp
import numpy as np
from jax import lax

HEADS = 8
HEAD_DIM = 128
BEAMS = 8
CAP = 2
HYP_DEV = 4
HYPS = 512
UTTS = 64
VOCAB = 16384


def draw_parent_beam(key, part):
    block_count = HYPS // HYP_DEV

    def draw_block(block_key, block_index):
        key_forced, key_pool, key_place = jax.random.split(block_key, 3)
        forced = jax.random.randint(key_forced, (), 1, BEAMS)
        offset_pool = jnp.concatenate([jnp.zeros((HYP_DEV,), jnp.int32), jnp.repeat(jnp.arange(1, BEAMS, dtype=jnp.int32), CAP)])
        shuffled = offset_pool[jax.random.permutation(key_pool, offset_pool.shape[0])]
        ordering = jnp.argsort((shuffled == forced).astype(jnp.int32), stable=True)
        remaining = shuffled[ordering][:HYP_DEV - CAP]
        offsets = jnp.concatenate([jnp.full((CAP,), forced, jnp.int32), remaining])
        offsets = offsets[jax.random.permutation(key_place, HYP_DEV)]
        own_beam = block_index * HYP_DEV // UTTS
        return ((own_beam - offsets) % BEAMS).astype(jnp.int32)
    block_keys = jax.random.split(jax.random.fold_in(key, 11), block_count)
    drawn = jax.vmap(draw_block)(block_keys, jnp.arange(block_count, dtype=jnp.int32))
    return drawn.reshape(HYPS).astype(jnp.int32)


def plant(values, rng, low, high):
    extent = values.shape
    place = [jax.random.randint(jax.random.fold_in(rng, axis), (), 0, extent[axis]) for axis in range(len(extent))]
    values = values.at[tuple(place)].set(low)
    longest = extent.index(max(extent))
    place[longest] = (place[longest] + 1) % extent[longest]
    return values.at[tuple(place)].set(high)


def block_levels(key, extent, shards, smallest, largest):
    level = 1.0
    for axis_at, blocks in shards:
        draws = jax.random.uniform(jax.random.fold_in(jax.random.fold_in(key, 6), axis_at), (blocks,), jnp.float32, smallest / len(shards), largest / len(shards))
        level = level * jnp.repeat(jnp.exp(draws), extent[axis_at] // blocks).reshape((-1,) + (1,) * (len(extent) - 1 - axis_at))
    return level


def rank_table(amount, lean):
    loads = [(1 << 20) // math.isqrt(grade ** lean) + 1 for grade in range(1, amount + 1)]
    deviation = 1 + sum(loads) // (1 << 30)
    return np.cumsum(np.array([max(1, weight // deviation) for weight in loads]))


def ranked_ids(key, dims, amount, slope):
    table = rank_table(amount, slope)
    ticket = jax.random.randint(jax.random.fold_in(key, 1), dims, 0, int(table[amount - 1]))
    grade = jnp.searchsorted(jnp.asarray(table, jnp.int32), ticket, side="right")
    return jax.random.permutation(jax.random.fold_in(key, 2), amount)[grade].astype(jnp.int32)


def gaussian(rng, extent, spread, limit, cuts=(), kind=jnp.bfloat16):
    level = block_levels(rng, extent, cuts, -0.22, 0.18) if cuts else 1.0
    values = jax.random.normal(rng, extent, jnp.float32) * spread * level
    return jnp.minimum(jnp.maximum(values, -limit), limit).astype(kind)


def setup_inputs(seed: int = 0, part: int = 0) -> dict:
    key_of = jax.random.split(jax.random.key(seed), 7)
    part_keys = jax.random.split(jax.random.fold_in(key_of[6], part), 7)
    states = gaussian(part_keys[0], (HYPS, HEADS, HEAD_DIM, HEAD_DIM), 0.5, 4.0, ((0, 128), (1, 2)), jnp.float32)
    parent_beam = draw_parent_beam(jax.random.fold_in(jax.random.fold_in(key_of[6], part), 71), part)
    next_token = plant(ranked_ids(part_keys[2], (HYPS,), VOCAB, 2), jax.random.fold_in(part_keys[2], 3), 0, VOCAB - 1).astype(jnp.int32)
    proj_table = gaussian(key_of[3], (VOCAB, HEADS, 5 * HEAD_DIM), 1.0, 6.0, ((0, 128), (1, 2)))
    gate_table = gaussian(key_of[4], (VOCAB, 3, HEADS), 1.5, 6.0, ((0, 128), (2, 2)))
    gain = jnp.clip(1.0 + 0.18 * jax.random.normal(key_of[5], (HEADS, HEAD_DIM), jnp.float32), 0.1, 1.9)
    return dict(states=states, parent_beam=parent_beam, next_token=next_token, proj_table=proj_table, gate_table=gate_table, gain=gain)


def unit_norm(vector):
    return vector * lax.rsqrt(lax.optimization_barrier(jnp.sum(vector * vector, axis=-1, keepdims=True)) + 1e-06)

def advance(parents, entries, gate_entries, gain):
    retain = jax.nn.sigmoid(gate_entries[:, 0, :])
    strengths = 2.0 * jax.nn.sigmoid(gate_entries[:, 1:, :])
    state_now = retain[:, :, None, None] * parents
    for reflect in range(2):
        key_unit = unit_norm(entries[:, :, 1 + reflect, :])
        value_row = entries[:, :, 3 + reflect, :]
        applied = jnp.einsum('nhvd,nhd->nhv', state_now, key_unit, precision=lax.Precision.HIGHEST)
        state_now = state_now - strengths[:, reflect, :, None, None] * (applied - value_row)[:, :, :, None] * key_unit[:, :, None, :]
    query_unit = unit_norm(entries[:, :, 0, :])
    readout = jnp.einsum('nhvd,nhd->nhv', state_now, query_unit, precision=lax.Precision.HIGHEST)
    normed = gain[None, :, :] * readout * lax.rsqrt(lax.optimization_barrier(jnp.mean(readout * readout, axis=-1, keepdims=True)) + 1e-05)
    return (normed.astype(jnp.bfloat16), state_now)

def reference(states, parent_beam, next_token, proj_table, gate_table, gain):
    hyp_index = jnp.arange(HYPS, dtype=jnp.int32)
    utterance = hyp_index % UTTS
    parent_hyp = (parent_beam * UTTS + utterance).astype(jnp.int32)
    parents = states[parent_hyp]
    entries = proj_table[next_token].astype(jnp.float32).reshape(HYPS, HEADS, 5, HEAD_DIM)
    gate_entries = gate_table[next_token].astype(jnp.float32)
    return advance(parents, entries, gate_entries, gain)
```

```python
import functools

import jax
import jax.numpy as jnp
from jax import lax
from jax.experimental import pallas as pl
from jax.experimental.pallas import tpu as pltpu
from jax.sharding import PartitionSpec as P

BEAMS = 8
ROW = 4
IDS = 8
LEVELS = 32767.0


def to(index):
    return dict(device_id={"beam": index}, device_id_type=pl.DeviceIdType.MESH)


def gather_kernel(count, states, ids, items, scales, table, q, qs, near, side, tile, sems, rsem):
    n = lax.axis_size("beam")
    me = lax.axis_index("beam")
    spacing = n // BEAMS
    rows = spacing // ROW
    my_beam, within = me // spacing, me % spacing
    row, col = within // ROW, within % ROW
    base = my_beam * spacing
    beam_peers = [(me + k * spacing) % n for k in range(1, BEAMS)]
    row_peers = [base + ((row + k) % rows) * ROW + col for k in range(1, rows)]
    col_peers = [base + row * ROW + (col + k) % ROW for k in range(1, ROW)]
    peers = beam_peers + row_peers + col_peers
    barrier = pltpu.get_barrier_semaphore()
    for p in peers:
        pl.semaphore_signal(barrier, inc=1, **to(p))
    pl.semaphore_wait(barrier, len(peers))

    copies = []
    at = [0]

    def send(src, dst, target):
        c = pltpu.make_async_remote_copy(
            src_ref=src, dst_ref=dst, send_sem=sems.at[at[0]], recv_sem=rsem.at[at[0]], **to(target)
        )
        at[0] += 1
        c.start()
        copies.append(c)
        return c

    def code(u):
        for h in range(states.shape[1]):
            x = states[u, h]
            top = jnp.maximum(jnp.max(jnp.abs(x), axis=0, keepdims=True), 1e-30)
            qs[u, h : h + 1, :] = top * (1.0 / LEVELS)
            q[u, h] = lax.round(
                x * (LEVELS / top), lax.RoundingMethod.TO_NEAREST_EVEN
            ).astype(jnp.int32).astype(jnp.int16)

    first = [send(ids, near.at[k], p) for k, p in enumerate(row_peers)]
    code(0)
    ways = (beam_peers[0], beam_peers[-1])
    for d in range(2):
        send(q.at[0], items.at[d * count], ways[d])
    for c in first:
        c.wait_recv()
    total = ids[...]
    for k in range(len(row_peers)):
        total = total + near[k]
    tile[0] = total
    for u in range(1, count):
        code(u)
    second = [send(tile.at[0], side.at[k], p) for k, p in enumerate(col_peers)]
    for c in second:
        c.wait_recv()
    for k in range(len(col_peers)):
        total = total + side[k]
    tile[1] = total
    for d in range(2):
        send(qs, scales.at[d], ways[d])
    for k, p in enumerate(beam_peers):
        send(tile.at[1], table.at[k + 1], p)
    for u in range(1, count):
        for d in range(2):
            send(q.at[u], items.at[d * count + u], ways[d])
    table[0] = total
    waited = set(map(id, first + second))
    for c in copies:
        c.wait_send()
        if id(c) not in waited:
            c.wait_recv()


def gather(states, ids):
    count, heads, size, _ = states.shape
    n = lax.axis_size("beam")
    rows = n // BEAMS // ROW
    sends = (rows - 1) + (ROW - 1) + (BEAMS - 1) + 2 * count + 2
    whole = pl.BlockSpec(memory_space=pltpu.VMEM)
    return pl.pallas_call(
        functools.partial(gather_kernel, count),
        out_shape=(
            jax.ShapeDtypeStruct((2 * count, heads, size, size), jnp.int16),
            jax.ShapeDtypeStruct((2, count, heads, size), jnp.float32),
            jax.ShapeDtypeStruct((BEAMS, 8, 128), jnp.int32),
        ),
        in_specs=[whole, whole],
        out_specs=(whole, whole, whole),
        scratch_shapes=[
            pltpu.VMEM((count, heads, size, size), jnp.int16),
            pltpu.VMEM((count, heads, size), jnp.float32),
            pltpu.VMEM((rows - 1, 8, 128), jnp.int32),
            pltpu.VMEM((ROW - 1, 8, 128), jnp.int32),
            pltpu.VMEM((2, 8, 128), jnp.int32),
            pltpu.SemaphoreType.DMA((sends,)),
            pltpu.SemaphoreType.DMA((sends,)),
        ],
        compiler_params=pltpu.CompilerParams(
            collective_id=0, has_side_effects=True, vmem_limit_bytes=24 << 20
        ),
    )(states, ids)


def lowest(row_of, beam, count):
    u = count - 1
    for k in range(count - 2, -1, -1):
        u = jnp.where(row_of(k) == beam, k, u)
    return u


def highest(row_of, beam, count):
    u = 0
    for k in range(1, count):
        u = jnp.where(row_of(k) == beam, k, u)
    return u


def relay_kernel(count, wants, states, items1, scales1, parents, *scratch):
    two, three, four, picked = scratch[0:2], scratch[2:4], scratch[4:6], scratch[6:8]
    two_s, three_s, four_s, picked_s = scratch[8:10], scratch[10:12], scratch[12:14], scratch[14:16]
    sems, rsem = scratch[16:]
    n = lax.axis_size("beam")
    me = lax.axis_index("beam")
    spacing = n // BEAMS
    my_beam = me // spacing
    ways = ((me + spacing) % n, (me + n - spacing) % n)
    barrier = pltpu.get_barrier_semaphore()
    for p in ways:
        pl.semaphore_signal(barrier, inc=1, **to(p))
    pl.semaphore_wait(barrier, 2)

    def beam(d):
        return (my_beam + BEAMS + d) % BEAMS

    def wanted_by(d):
        return lambda u: wants[(BEAMS - d) % BEAMS, u]

    copies = []
    at = [0]

    def send(src, dst, way):
        c = pltpu.make_async_remote_copy(
            src_ref=src, dst_ref=dst, send_sem=sems.at[at[0]], recv_sem=rsem.at[at[0]], **to(ways[way])
        )
        at[0] += 1
        c.start()
        copies.append(c)
        return c

    step2 = [[send(scales1.at[d], two_s[d], d)] for d in range(2)]
    for u in range(count):
        for d in range(2):
            step2[d].append(send(items1.at[d * count + u], two[d].at[u], d))
    step3 = []
    for d in range(2):
        for c in step2[d]:
            c.wait_recv()
        sign = 1 if d == 0 else -1
        origin = beam(-2 * sign)
        nearer = wanted_by(sign)
        farther = wanted_by(2 * sign)
        end = lowest if d == 0 else highest
        chosen = (
            lowest(nearer, origin, count), highest(nearer, origin, count), end(farther, origin, count)
        )
        for s, u in enumerate(chosen):
            picked_s[d][s] = two_s[d][u]
            picked[d][s] = two[d][u]
        step3.append([send(picked_s[d], three_s[d], d)])
        for s in (2, 0, 1):
            step3[d].append(send(picked[d].at[s], three[d].at[s], d))
    step4 = []
    for d in range(2):
        step3[d][0].wait_recv()
        step4.append(send(three_s[d].at[2], four_s[d].at[0], d))
        step3[d][1].wait_recv()
        step4.append(send(three[d].at[2], four[d].at[0], d))
    for d in range(2):
        for c in step3[d][2:]:
            c.wait_recv()
    for c in step4:
        c.wait_recv()
    mine = wanted_by(0)
    for u in range(count):
        offset = (my_beam + BEAMS - mine(u)) % BEAMS
        third = [jnp.where(lowest(mine, beam(d), count) == u, 0, 1) for d in (-3, 3)]
        middle = lowest(mine, beam(4), count) == u
        one = jnp.where(offset == BEAMS - 1, count + u, u)
        for h in range(states.shape[1]):
            x = states[u, h]

            def take(x, when, code, scale):
                return jnp.where(when, code.astype(jnp.int32).astype(jnp.float32) * scale, x)

            x = take(
                x, (offset == 1) | (offset == BEAMS - 1),
                items1[one, h], scales1[one // count, u, h : h + 1, :],
            )
            for d in range(2):
                x = take(
                    x, offset == (2, BEAMS - 2)[d], two[d][u, h], two_s[d][u, h : h + 1, :]
                )
                x = take(
                    x, offset == (3, BEAMS - 3)[d],
                    three[d][third[d], h], three_s[d][third[d], h : h + 1, :],
                )
                x = take(
                    x, (offset == 4) & (middle if d == 0 else jnp.logical_not(middle)),
                    four[d][0, h], four_s[d][0, h : h + 1, :],
                )
            parents[u, h] = x
    for c in copies:
        c.wait_send()


def relay(wants, states, items1, scales1):
    count, heads, size, _ = states.shape
    sends = 2 * (1 + count) + 2 * 4 + 4
    whole = pl.BlockSpec(memory_space=pltpu.VMEM)
    kept = [count, count, 3, 3, 1, 1, 3, 3]
    return pl.pallas_call(
        functools.partial(relay_kernel, count),
        out_shape=jax.ShapeDtypeStruct(states.shape, jnp.float32),
        in_specs=[pl.BlockSpec(memory_space=pltpu.SMEM), whole, whole, whole],
        out_specs=whole,
        scratch_shapes=[
            *(pltpu.VMEM((k, heads, size, size), jnp.int16) for k in kept),
            *(pltpu.VMEM((k, heads, size), jnp.float32) for k in kept),
            pltpu.SemaphoreType.DMA((sends,)),
            pltpu.SemaphoreType.DMA((sends,)),
        ],
        cost_estimate=pl.CostEstimate(flops=10**9, bytes_accessed=6 << 20, transcendentals=0),
        compiler_params=pltpu.CompilerParams(
            collective_id=1, has_side_effects=True, vmem_limit_bytes=24 << 20
        ),
    )(wants, states, items1, scales1)


def advance_kernel(parents, entries, gates, gain, readout, new_states):
    heads, size = parents.shape[1], parents.shape[2]
    eye = (
        lax.broadcasted_iota(jnp.int32, (size, size), 0)
        == lax.broadcasted_iota(jnp.int32, (size, size), 1)
    ).astype(jnp.float32)
    gate = jax.nn.sigmoid(gates[0])
    rows = []
    for h in range(heads):

        def entry(k):
            return entries[0, h * 5 + k : h * 5 + k + 1, :]

        def unit(x):
            return x * lax.rsqrt(jnp.sum(x * x, axis=-1, keepdims=True) + 1e-06)

        def level(k):
            return gate[k * heads + h : k * heads + h + 1, :]

        state = level(0) * parents[0, h]
        for j in range(2):
            key = unit(entry(1 + j))
            gap = jnp.sum(state * key - eye * entry(3 + j), axis=-1, keepdims=True)
            state = state - gap * (2.0 * level(1 + j) * key)
        new_states[0, h] = state
        out = jnp.sum(state * unit(entry(0)), axis=-1, keepdims=True)
        row = jnp.sum(eye * out, axis=0, keepdims=True)
        scale = lax.rsqrt(jnp.sum(row * row, axis=-1, keepdims=True) * (1.0 / size) + 1e-05)
        rows.append(gain[h : h + 1, :] * row * scale)
    readout[0] = jnp.concatenate(rows, axis=0).astype(jnp.bfloat16)


def advance(parents, entries, gates, gain):
    count, heads, size, _ = parents.shape
    return pl.pallas_call(
        advance_kernel,
        grid=(count,),
        out_shape=(
            jax.ShapeDtypeStruct((count, heads, size), jnp.bfloat16),
            jax.ShapeDtypeStruct(parents.shape, jnp.float32),
        ),
        in_specs=[
            pl.BlockSpec((1, heads, size, size), lambda i: (i, 0, 0, 0)),
            pl.BlockSpec((1, heads * 5, size), lambda i: (i, 0, 0)),
            pl.BlockSpec((1, 3 * heads, size), lambda i: (i, 0, 0)),
            pl.BlockSpec((heads, size), lambda i: (0, 0)),
        ],
        out_specs=(
            pl.BlockSpec((1, heads, size), lambda i: (i, 0, 0)),
            pl.BlockSpec((1, heads, size, size), lambda i: (i, 0, 0, 0)),
        ),
    )(parents, entries, gates, gain)


def local(states, parent_beam, next_token, proj_table, gate_table, gain):
    count, heads, size, _ = states.shape
    devices = lax.axis_size("beam")
    spacing = devices // BEAMS
    position = lax.axis_index("beam")
    my_beam, within = position // spacing, position % spacing
    lanes = jnp.zeros((128,), jnp.int32)
    mine = jnp.concatenate([next_token, parent_beam])
    lanes = lax.dynamic_update_slice(lanes, mine, (within * 2 * count,))
    ids = jnp.broadcast_to(lanes[None, :], (8, 128))
    items1, scales1, table = gather(states, ids)
    every = table[:, 0, :].reshape(BEAMS, spacing, 2 * count)
    wants = lax.dynamic_slice_in_dim(every, within, 1, axis=1)[:, 0, count:]
    order = (my_beam + BEAMS - jnp.arange(BEAMS)) % BEAMS
    tokens = jnp.take(every[:, :, :count], order, axis=0).reshape(-1)

    vocab_rows = proj_table.shape[0]
    wide = 5 * size
    padded = jnp.concatenate(
        [
            proj_table.transpose(1, 0, 2),
            gate_table.transpose(2, 0, 1),
            jnp.zeros((heads, vocab_rows, size - 3), proj_table.dtype),
        ],
        axis=2,
    ).reshape(heads * vocab_rows, wide + size)
    wanted = jnp.repeat(tokens - position * vocab_rows, heads)
    head_at = jnp.arange(heads * vocab_rows, dtype=jnp.int32) // vocab_rows
    row_at = jnp.arange(heads * vocab_rows, dtype=jnp.int32) % vocab_rows
    own_head = jnp.arange(wanted.shape[0], dtype=jnp.int32) % heads
    onehot = (
        (wanted[:, None] == row_at[None, :]) & (own_head[:, None] == head_at[None, :])
    ).astype(jnp.bfloat16)
    looked = jnp.dot(onehot, padded, preferred_element_type=jnp.float32).astype(jnp.bfloat16)
    arrived = lax.psum_scatter(looked, "beam", scatter_dimension=0, tiled=True)
    parents = relay(wants, states, items1, scales1)
    arrived = arrived.astype(jnp.float32).reshape(count, heads, wide + size)
    entries = arrived[:, :, :wide].reshape(count, heads * 5, size)
    gates = arrived[:, :, wide : wide + 3].transpose(0, 2, 1).reshape(count, 3 * heads)
    gates = jnp.broadcast_to(gates[:, :, None], (count, 3 * heads, size))
    return advance(parents, entries, gates, gain)


def solution(mesh):
    return jax.shard_map(
        local,
        mesh=mesh,
        in_specs=(
            P(("groups", "beam"), "mp", None, None),
            P(("groups", "beam")),
            P(("groups", "beam")),
            P("beam", "mp", None),
            P("beam", None, "mp"),
            P("mp", None),
        ),
        out_specs=(P(("groups", "beam"), "mp", None), P(("groups", "beam"), "mp", None, None)),
        check_vma=False,
    )
```

```python
import functools

import jax
import jax.numpy as jnp
from jax import lax
from jax.experimental import pallas as pl
from jax.experimental.pallas import tpu as pltpu
from jax.sharding import PartitionSpec as P

BEAMS = 8
ROW = 4
IDS = 8
LEVELS = 32767.0


def to(index):
    return dict(device_id={"beam": index}, device_id_type=pl.DeviceIdType.MESH)


def gather_kernel(count, states, ids, items, scales, table, q, qs, near, side, tile, sems, rsem):
    n = lax.axis_size("beam")
    me = lax.axis_index("beam")
    spacing = n // BEAMS
    rows = spacing // ROW
    my_beam, within = me // spacing, me % spacing
    row, col = within // ROW, within % ROW
    base = my_beam * spacing
    beam_peers = [(me + k * spacing) % n for k in range(1, BEAMS)]
    row_peers = [base + ((row + k) % rows) * ROW + col for k in range(1, rows)]
    col_peers = [base + row * ROW + (col + k) % ROW for k in range(1, ROW)]
    peers = beam_peers + row_peers + col_peers
    barrier = pltpu.get_barrier_semaphore()
    for p in peers:
        pl.semaphore_signal(barrier, inc=1, **to(p))
    pl.semaphore_wait(barrier, len(peers))

    copies = []
    at = [0]

    def send(src, dst, target):
        c = pltpu.make_async_remote_copy(
            src_ref=src, dst_ref=dst, send_sem=sems.at[at[0]], recv_sem=rsem.at[at[0]], **to(target)
        )
        at[0] += 1
        c.start()
        copies.append(c)
        return c

    def code(u):
        for h in range(states.shape[1]):
            x = states[u, h]
            top = jnp.maximum(jnp.max(jnp.abs(x), axis=0, keepdims=True), 1e-30)
            qs[u, h : h + 1, :] = top * (1.0 / LEVELS)
            q[u, h] = lax.round(
                x * (LEVELS / top), lax.RoundingMethod.TO_NEAREST_EVEN
            ).astype(jnp.int32).astype(jnp.int16)

    first = [send(ids, near.at[k], p) for k, p in enumerate(row_peers)]
    code(0)
    ways = (beam_peers[0], beam_peers[-1])
    for d in range(2):
        send(q.at[0], items.at[d * count], ways[d])
    for c in first:
        c.wait_recv()
    total = ids[...]
    for k in range(len(row_peers)):
        total = total + near[k]
    tile[0] = total
    for u in range(1, count):
        code(u)
    second = [send(tile.at[0], side.at[k], p) for k, p in enumerate(col_peers)]
    for c in second:
        c.wait_recv()
    for k in range(len(col_peers)):
        total = total + side[k]
    tile[1] = total
    for d in range(2):
        send(qs, scales.at[d], ways[d])
    for k, p in enumerate(beam_peers):
        send(tile.at[1], table.at[k + 1], p)
    for u in range(1, count):
        for d in range(2):
            send(q.at[u], items.at[d * count + u], ways[d])
    table[0] = total
    waited = set(map(id, first + second))
    for c in copies:
        c.wait_send()
        if id(c) not in waited:
            c.wait_recv()


def gather(states, ids):
    count, heads, size, _ = states.shape
    n = lax.axis_size("beam")
    rows = n // BEAMS // ROW
    sends = (rows - 1) + (ROW - 1) + (BEAMS - 1) + 2 * count + 2
    whole = pl.BlockSpec(memory_space=pltpu.VMEM)
    return pl.pallas_call(
        functools.partial(gather_kernel, count),
        out_shape=(
            jax.ShapeDtypeStruct((2 * count, heads, size, size), jnp.int16),
            jax.ShapeDtypeStruct((2, count, heads, size), jnp.float32),
            jax.ShapeDtypeStruct((BEAMS, 8, 128), jnp.int32),
        ),
        in_specs=[whole, whole],
        out_specs=(whole, whole, whole),
        scratch_shapes=[
            pltpu.VMEM((count, heads, size, size), jnp.int16),
            pltpu.VMEM((count, heads, size), jnp.float32),
            pltpu.VMEM((rows - 1, 8, 128), jnp.int32),
            pltpu.VMEM((ROW - 1, 8, 128), jnp.int32),
            pltpu.VMEM((2, 8, 128), jnp.int32),
            pltpu.SemaphoreType.DMA((sends,)),
            pltpu.SemaphoreType.DMA((sends,)),
        ],
        compiler_params=pltpu.CompilerParams(
            collective_id=0, has_side_effects=True, vmem_limit_bytes=24 << 20
        ),
    )(states, ids)


def lowest(row_of, beam, count):
    u = count - 1
    for k in range(count - 2, -1, -1):
        u = jnp.where(row_of(k) == beam, k, u)
    return u


def highest(row_of, beam, count):
    u = 0
    for k in range(1, count):
        u = jnp.where(row_of(k) == beam, k, u)
    return u


def relay_kernel(count, wants, states, items1, scales1, looked, parents, arrived, *scratch):
    two, three, four, picked = scratch[0:2], scratch[2:4], scratch[4:6], scratch[6:8]
    two_s, three_s, four_s, picked_s = scratch[8:10], scratch[10:12], scratch[12:14], scratch[14:16]
    opposite_half, from_cols, from_rows = scratch[16:18], scratch[18:20], scratch[20:-10]
    part_sum, hops, from_beam = scratch[-10:-8], scratch[-8:-6], scratch[-6:-4]
    col_sum, row_sum, sems, rsem = scratch[-4:]
    n = lax.axis_size("beam")
    me = lax.axis_index("beam")
    spacing = n // BEAMS
    my_beam = me // spacing
    rows = spacing // ROW
    within = me % spacing
    row, col = within // ROW, within % ROW
    base = my_beam * spacing
    ways = ((me + spacing) % n, (me + n - spacing) % n)
    cols = ((col + 1) % ROW, (col + ROW - 1) % ROW)
    across = (col + 2) % ROW
    col_ways = [base + row * ROW + c for c in cols]
    row_ids = [(row + k) % rows for k in range(1, rows)]
    row_peers = [base + r * ROW + col for r in row_ids]
    barrier = pltpu.get_barrier_semaphore()
    peers = [*ways, *col_ways, *row_peers]
    for p in peers:
        pl.semaphore_signal(barrier, inc=1, **to(p))
    pl.semaphore_wait(barrier, len(peers))

    def beam(d):
        return (my_beam + BEAMS + d) % BEAMS

    def wanted_by(d):
        return lambda u: wants[(BEAMS - d) % BEAMS, u]

    copies = []
    at = [0]

    def send_to(src, dst, target):
        c = pltpu.make_async_remote_copy(
            src_ref=src, dst_ref=dst, send_sem=sems.at[at[0]], recv_sem=rsem.at[at[0]], **to(target)
        )
        at[0] += 1
        c.start()
        copies.append(c)
        return c

    def send(src, dst, way):
        return send_to(src, dst, ways[way])

    def add(dst, *srcs):
        def step(i, _):
            x = srcs[0][i]
            for y in srcs[1:]:
                x = x + y[i]
            dst[i] = x
            return 0

        lax.fori_loop(0, dst.shape[0], step, 0)

    blocks = BEAMS * rows
    half = blocks // 2
    halves = (pl.ds(0, half), pl.ds(half, half))
    opposite, straight = [], []
    for d in range(2):
        opposite.append(send_to(looked.at[across, halves[d]], opposite_half[d], col_ways[d]))
    for d in range(2):
        straight.append(
            send_to(
                looked.at[cols[d], halves[1 - d]], from_cols[d].at[halves[1 - d]], col_ways[d]
            )
        )
    step2 = [[send(scales1.at[d], two_s[d], d)] for d in range(2)]
    for u in range(count):
        for d in range(2):
            step2[d].append(send(items1.at[d * count + u], two[d].at[u], d))
    for d in range(2):
        opposite[d].wait()
        part = part_sum[d]
        add(part, opposite_half[d], looked.at[cols[d], halves[d]])
        straight.append(send_to(part, from_cols[d].at[halves[d]], col_ways[d]))
    for c in straight:
        c.wait_recv()
    add(col_sum, looked.at[col], from_cols[0], from_cols[1])
    row_sends = [
        send_to(col_sum.at[pl.ds(r * BEAMS, BEAMS)], from_rows[k], p)
        for k, (r, p) in enumerate(zip(row_ids, row_peers))
    ]
    step3 = []
    chosen = []
    for d in range(2):
        for c in step2[d]:
            c.wait_recv()
        sign = 1 if d == 0 else -1
        origin = beam(-2 * sign)
        nearer = wanted_by(sign)
        farther = wanted_by(2 * sign)
        end = lowest if d == 0 else highest
        chosen.append((
            lowest(nearer, origin, count), highest(nearer, origin, count), end(farther, origin, count)
        ))
        for s in range(3):
            picked_s[d][s] = two_s[d][chosen[d][s]]
        for s in range(3):
            picked[d][s] = two[d][chosen[d][s]]
        step3.append([send(picked_s[d], three_s[d], d)])
        step3[d].append(send(picked[d].at[2], three[d].at[2], d))
    for c in row_sends:
        c.wait_recv()
    add(row_sum, col_sum.at[pl.ds(row * BEAMS, BEAMS)], *from_rows)
    reach = (BEAMS // 2, BEAMS // 2 - 1)

    def block(d, distance):
        return (BEAMS - distance) % BEAMS if d == 0 else distance

    passed = [[] for _ in range(2)]

    def pass_on(d):
        k = len(passed[d])
        if k == reach[d]:
            return
        at_block = block(d, reach[d] - k)
        if k == 0:
            src = row_sum.at[at_block]
        else:
            passed[d][k - 1].wait_recv()
            hops[d][k] = row_sum[at_block] + from_beam[d][k - 1]
            src = hops[d].at[k]
        passed[d].append(send(src, from_beam[d].at[k], d))

    for d in range(2):
        pass_on(d)
        step3[d].append(send(picked[d].at[0], three[d].at[0], d))
    for d in range(2):
        pass_on(d)
        step3[d].append(send(picked[d].at[1], three[d].at[1], d))
    step4 = []
    for d in range(2):
        step3[d][0].wait_recv()
        step4.append(send(three_s[d].at[2], four_s[d].at[0], d))
        step3[d][1].wait_recv()
        step4.append(send(three[d].at[2], four[d].at[0], d))
        pass_on(d)
    for d in range(2):
        pass_on(d)
    for d in range(2):
        for c in step3[d][2:]:
            c.wait_recv()
    for c in step4:
        c.wait_recv()
    for d in range(2):
        passed[d][-1].wait_recv()
    arrived[...] = row_sum[0] + from_beam[0][reach[0] - 1] + from_beam[1][reach[1] - 1]
    mine = wanted_by(0)
    for u in range(count):
        offset = (my_beam + BEAMS - mine(u)) % BEAMS
        third = [jnp.where(lowest(mine, beam(d), count) == u, 0, 1) for d in (-3, 3)]
        middle = lowest(mine, beam(4), count) == u
        one = jnp.where(offset == BEAMS - 1, count + u, u)
        for h in range(states.shape[1]):
            x = states[u, h]

            def take(x, when, code, scale):
                return jnp.where(when, code.astype(jnp.int32).astype(jnp.float32) * scale, x)

            x = take(
                x, (offset == 1) | (offset == BEAMS - 1),
                items1[one, h], scales1[one // count, u, h : h + 1, :],
            )
            for d in range(2):
                x = take(
                    x, offset == (2, BEAMS - 2)[d], two[d][u, h], two_s[d][u, h : h + 1, :]
                )
                x = take(
                    x, offset == (3, BEAMS - 3)[d],
                    three[d][third[d], h], three_s[d][third[d], h : h + 1, :],
                )
                x = take(
                    x, (offset == 4) & (middle if d == 0 else jnp.logical_not(middle)),
                    four[d][0, h], four_s[d][0, h : h + 1, :],
                )
            parents[u, h] = x
    for c in copies:
        if id(c) not in set(map(id, opposite)):
            c.wait_send()


def relay(wants, states, items1, scales1, looked):
    count, heads, size, _ = states.shape
    blocks, height, width = looked.shape[1:]
    rows = blocks // BEAMS
    sends = 2 * (1 + count) + 2 * 4 + 4 + 6 + (rows - 1) + BEAMS - 1
    whole = pl.BlockSpec(memory_space=pltpu.VMEM)
    kept = [count, count, 3, 3, 1, 1, 3, 3]
    parts = [blocks // 2] * 2 + [blocks] * 2 + [BEAMS] * (rows - 1) + [blocks // 2] * 2
    parts += [BEAMS // 2] * 4 + [blocks, BEAMS]
    return pl.pallas_call(
        functools.partial(relay_kernel, count),
        out_shape=(
            jax.ShapeDtypeStruct(states.shape, jnp.float32),
            jax.ShapeDtypeStruct((height, width), looked.dtype),
        ),
        in_specs=[pl.BlockSpec(memory_space=pltpu.SMEM), whole, whole, whole, whole],
        out_specs=(whole, whole),
        scratch_shapes=[
            *(pltpu.VMEM((k, heads, size, size), jnp.int16) for k in kept),
            *(pltpu.VMEM((k, heads, size), jnp.float32) for k in kept),
            *(pltpu.VMEM((k, height, width), looked.dtype) for k in parts),
            pltpu.SemaphoreType.DMA((sends,)),
            pltpu.SemaphoreType.DMA((sends,)),
        ],
        compiler_params=pltpu.CompilerParams(
            collective_id=1, has_side_effects=True, vmem_limit_bytes=40 << 20
        ),
    )(wants, states, items1, scales1, looked)


def advance_kernel(parents, entries, gates, gain, readout, new_states):
    heads, size = parents.shape[1], parents.shape[2]
    eye = (
        lax.broadcasted_iota(jnp.int32, (size, size), 0)
        == lax.broadcasted_iota(jnp.int32, (size, size), 1)
    ).astype(jnp.float32)
    gate = jax.nn.sigmoid(gates[0])
    rows = []
    for h in range(heads):

        def entry(k):
            return entries[0, h * 5 + k : h * 5 + k + 1, :]

        def unit(x):
            return x * lax.rsqrt(jnp.sum(x * x, axis=-1, keepdims=True) + 1e-06)

        def level(k):
            return gate[k * heads + h : k * heads + h + 1, :]

        state = level(0) * parents[0, h]
        for j in range(2):
            key = unit(entry(1 + j))
            gap = jnp.sum(state * key - eye * entry(3 + j), axis=-1, keepdims=True)
            state = state - gap * (2.0 * level(1 + j) * key)
        new_states[0, h] = state
        out = jnp.sum(state * unit(entry(0)), axis=-1, keepdims=True)
        row = jnp.sum(eye * out, axis=0, keepdims=True)
        scale = lax.rsqrt(jnp.sum(row * row, axis=-1, keepdims=True) * (1.0 / size) + 1e-05)
        rows.append(gain[h : h + 1, :] * row * scale)
    readout[0] = jnp.concatenate(rows, axis=0).astype(jnp.bfloat16)


def advance(parents, entries, gates, gain):
    count, heads, size, _ = parents.shape
    return pl.pallas_call(
        advance_kernel,
        grid=(count,),
        out_shape=(
            jax.ShapeDtypeStruct((count, heads, size), jnp.bfloat16),
            jax.ShapeDtypeStruct(parents.shape, jnp.float32),
        ),
        in_specs=[
            pl.BlockSpec((1, heads, size, size), lambda i: (i, 0, 0, 0)),
            pl.BlockSpec((1, heads * 5, size), lambda i: (i, 0, 0)),
            pl.BlockSpec((1, 3 * heads, size), lambda i: (i, 0, 0)),
            pl.BlockSpec((heads, size), lambda i: (0, 0)),
        ],
        out_specs=(
            pl.BlockSpec((1, heads, size), lambda i: (i, 0, 0)),
            pl.BlockSpec((1, heads, size, size), lambda i: (i, 0, 0, 0)),
        ),
    )(parents, entries, gates, gain)


def local(states, parent_beam, next_token, proj_table, gate_table, gain):
    count, heads, size, _ = states.shape
    devices = lax.axis_size("beam")
    spacing = devices // BEAMS
    position = lax.axis_index("beam")
    my_beam, within = position // spacing, position % spacing
    lanes = jnp.zeros((128,), jnp.int32)
    mine = jnp.concatenate([next_token, parent_beam])
    lanes = lax.dynamic_update_slice(lanes, mine, (within * 2 * count,))
    ids = jnp.broadcast_to(lanes[None, :], (8, 128))
    items1, scales1, table = gather(states, ids)
    every = table[:, 0, :].reshape(BEAMS, spacing, 2 * count)
    wants = lax.dynamic_slice_in_dim(every, within, 1, axis=1)[:, 0, count:]
    tokens = every[:, :, :count].reshape(BEAMS, spacing // ROW, ROW, count).transpose(2, 1, 0, 3).reshape(-1)

    vocab_rows = proj_table.shape[0]
    wide = 5 * size
    padded = jnp.concatenate(
        [
            proj_table.transpose(1, 0, 2),
            gate_table.transpose(2, 0, 1),
            jnp.zeros((heads, vocab_rows, size - 3), proj_table.dtype),
        ],
        axis=2,
    ).reshape(heads * vocab_rows, wide + size)
    wanted = jnp.repeat(tokens - position * vocab_rows, heads)
    head_at = jnp.arange(heads * vocab_rows, dtype=jnp.int32) // vocab_rows
    row_at = jnp.arange(heads * vocab_rows, dtype=jnp.int32) % vocab_rows
    own_head = jnp.arange(wanted.shape[0], dtype=jnp.int32) % heads
    onehot = (
        (wanted[:, None] == row_at[None, :]) & (own_head[:, None] == head_at[None, :])
    ).astype(jnp.bfloat16)
    looked = jnp.dot(onehot, padded, preferred_element_type=jnp.float32).astype(jnp.bfloat16)
    looked = looked.reshape(ROW, devices // ROW, count * heads, wide + size)
    parents, arrived = relay(wants, states, items1, scales1, looked)
    arrived = arrived.astype(jnp.float32).reshape(count, heads, wide + size)
    entries = arrived[:, :, :wide].reshape(count, heads * 5, size)
    gates = arrived[:, :, wide : wide + 3].transpose(0, 2, 1).reshape(count, 3 * heads)
    gates = jnp.broadcast_to(gates[:, :, None], (count, 3 * heads, size))
    return advance(parents, entries, gates, gain)


def solution(mesh):
    return jax.shard_map(
        local,
        mesh=mesh,
        in_specs=(
            P(("groups", "beam"), "mp", None, None),
            P(("groups", "beam")),
            P(("groups", "beam")),
            P("beam", "mp", None),
            P("beam", None, "mp"),
            P("mp", None),
        ),
        out_specs=(P(("groups", "beam"), "mp", None), P(("groups", "beam"), "mp", None, None)),
        check_vma=False,
    )
```

```python
import functools

import jax
import jax.numpy as jnp
from jax import lax
from jax.experimental import pallas as pl
from jax.experimental.pallas import tpu as pltpu
from jax.sharding import PartitionSpec as P

BEAMS = 8
ROW = 4
IDS = 8
LEVELS = 32767.0
EARLY = 2


def to(index):
    return dict(device_id={"beam": index}, device_id_type=pl.DeviceIdType.MESH)


def gather_kernel(count, states, ids, items, scales, table, late, q, qs, near, side, tile, sems, rsem):
    n = lax.axis_size("beam")
    me = lax.axis_index("beam")
    spacing = n // BEAMS
    rows = spacing // ROW
    my_beam, within = me // spacing, me % spacing
    row, col = within // ROW, within % ROW
    base = my_beam * spacing
    beam_peers = [(me + k * spacing) % n for k in range(1, BEAMS)]
    row_peers = [base + ((row + k) % rows) * ROW + col for k in range(1, rows)]
    col_peers = [base + row * ROW + (col + k) % ROW for k in range(1, ROW)]
    peers = beam_peers + row_peers + col_peers
    barrier = pltpu.get_barrier_semaphore()
    for p in peers:
        pl.semaphore_signal(barrier, inc=1, **to(p))
    pl.semaphore_wait(barrier, len(peers))

    copies = []
    at = [0]

    def send(src, dst, target):
        c = pltpu.make_async_remote_copy(
            src_ref=src, dst_ref=dst, send_sem=sems.at[at[0]], recv_sem=rsem.at[at[0]], **to(target)
        )
        at[0] += 1
        c.start()
        copies.append(c)
        return c

    def code(u):
        for h in range(states.shape[1]):
            x = states[u, h]
            top = jnp.maximum(jnp.max(jnp.abs(x), axis=0, keepdims=True), 1e-30)
            qs[u, h : h + 1, :] = top * (1.0 / LEVELS)
            code_to = q.at[u] if u < EARLY else late.at[u - EARLY]
            code_to[h] = lax.round(
                x * (LEVELS / top), lax.RoundingMethod.TO_NEAREST_EVEN
            ).astype(jnp.int32).astype(jnp.int16)

    first = [send(ids, near.at[k], p) for k, p in enumerate(row_peers)]
    code(0)
    ways = (beam_peers[0], beam_peers[-1])
    for d in range(2):
        send(q.at[0], items.at[d * EARLY], ways[d])
    for c in first:
        c.wait_recv()
    total = ids[...]
    for k in range(len(row_peers)):
        total = total + near[k]
    tile[0] = total
    for u in range(1, count):
        code(u)
    second = [send(tile.at[0], side.at[k], p) for k, p in enumerate(col_peers)]
    for c in second:
        c.wait_recv()
    for k in range(len(col_peers)):
        total = total + side[k]
    tile[1] = total
    for d in range(2):
        send(qs, scales.at[d], ways[d])
    for k, p in enumerate(beam_peers):
        send(tile.at[1], table.at[k + 1], p)
    for u in range(1, EARLY):
        for d in range(2):
            send(q.at[u], items.at[d * EARLY + u], ways[d])
    table[0] = total
    waited = set(map(id, first + second))
    for c in copies:
        c.wait_send()
        if id(c) not in waited:
            c.wait_recv()


def gather(states, ids):
    count, heads, size, _ = states.shape
    n = lax.axis_size("beam")
    rows = n // BEAMS // ROW
    sends = (rows - 1) + (ROW - 1) + (BEAMS - 1) + 2 * EARLY + 2
    whole = pl.BlockSpec(memory_space=pltpu.VMEM)
    return pl.pallas_call(
        functools.partial(gather_kernel, count),
        out_shape=(
            jax.ShapeDtypeStruct((2 * EARLY, heads, size, size), jnp.int16),
            jax.ShapeDtypeStruct((2, count, heads, size), jnp.float32),
            jax.ShapeDtypeStruct((BEAMS, 8, 128), jnp.int32),
            jax.ShapeDtypeStruct((count - EARLY, heads, size, size), jnp.int16),
        ),
        in_specs=[whole, whole],
        out_specs=(whole, whole, whole, whole),
        scratch_shapes=[
            pltpu.VMEM((EARLY, heads, size, size), jnp.int16),
            pltpu.VMEM((count, heads, size), jnp.float32),
            pltpu.VMEM((rows - 1, 8, 128), jnp.int32),
            pltpu.VMEM((ROW - 1, 8, 128), jnp.int32),
            pltpu.VMEM((2, 8, 128), jnp.int32),
            pltpu.SemaphoreType.DMA((sends,)),
            pltpu.SemaphoreType.DMA((sends,)),
        ],
        compiler_params=pltpu.CompilerParams(
            collective_id=0, has_side_effects=True, vmem_limit_bytes=24 << 20
        ),
    )(states, ids)


def lowest(row_of, beam, count):
    u = count - 1
    for k in range(count - 2, -1, -1):
        u = jnp.where(row_of(k) == beam, k, u)
    return u


def highest(row_of, beam, count):
    u = 0
    for k in range(1, count):
        u = jnp.where(row_of(k) == beam, k, u)
    return u


def advance(state, entry, gain):
    size = state.shape[0]
    eye = (
        lax.broadcasted_iota(jnp.int32, (size, size), 0)
        == lax.broadcasted_iota(jnp.int32, (size, size), 1)
    ).astype(jnp.float32)

    def vector(k):
        return entry(slice(k * size, (k + 1) * size))

    def unit(x):
        return x * lax.rsqrt(jnp.sum(x * x, axis=-1, keepdims=True) + 1e-06)

    def gate(k):
        x = entry(slice(5 * size + k, 5 * size + k + 1))
        return 1.0 / (1.0 + jnp.exp(-jnp.broadcast_to(x, (1, size))))

    state = gate(0) * state
    for j in range(2):
        key = unit(vector(1 + j))
        gap = jnp.sum(state * key - eye * vector(3 + j), axis=-1, keepdims=True)
        state = state - gap * (2.0 * gate(1 + j) * key)
    out = jnp.sum(state * unit(vector(0)), axis=-1, keepdims=True)
    row = jnp.sum(eye * out, axis=0, keepdims=True)
    scale = lax.rsqrt(jnp.sum(row * row, axis=-1, keepdims=True) * (1.0 / size) + 1e-05)
    return state, gain * row * scale


def relay_kernel(
    count, wants, states, items1, scales1, late, looked, gain, readout, new_states, *scratch
):
    two, three, four, picked = scratch[0:2], scratch[2:4], scratch[4:6], scratch[6:8]
    two_s, three_s, four_s, picked_s = scratch[8:10], scratch[10:12], scratch[12:14], scratch[14:16]
    one = scratch[16:18]
    opposite_half, from_cols, from_rows = scratch[18:20], scratch[20:22], scratch[22:-11]
    part_sum, hops, from_beam = scratch[-11:-9], scratch[-9:-7], scratch[-7:-5]
    col_sum, row_sum, entries, sems, rsem = scratch[-5:]
    n = lax.axis_size("beam")
    me = lax.axis_index("beam")
    spacing = n // BEAMS
    my_beam = me // spacing
    rows = spacing // ROW
    within = me % spacing
    row, col = within // ROW, within % ROW
    base = my_beam * spacing
    ways = ((me + spacing) % n, (me + n - spacing) % n)
    cols = ((col + 1) % ROW, (col + ROW - 1) % ROW)
    across = (col + 2) % ROW
    col_ways = [base + row * ROW + c for c in cols]
    row_ids = [(row + k) % rows for k in range(1, rows)]
    row_peers = [base + r * ROW + col for r in row_ids]
    barrier = pltpu.get_barrier_semaphore()
    peers = [*ways, *col_ways, *row_peers]
    for p in peers:
        pl.semaphore_signal(barrier, inc=1, **to(p))
    pl.semaphore_wait(barrier, len(peers))

    def beam(d):
        return (my_beam + BEAMS + d) % BEAMS

    def wanted_by(d):
        return lambda u: wants[(BEAMS - d) % BEAMS, u]

    copies = []
    at = [0]

    def send_to(src, dst, target):
        c = pltpu.make_async_remote_copy(
            src_ref=src, dst_ref=dst, send_sem=sems.at[at[0]], recv_sem=rsem.at[at[0]], **to(target)
        )
        at[0] += 1
        c.start()
        copies.append(c)
        return c

    def send(src, dst, way):
        return send_to(src, dst, ways[way])

    def add(dst, *srcs):
        def step(i, _):
            x = srcs[0][i]
            for y in srcs[1:]:
                x = x + y[i]
            dst[i] = x
            return 0

        lax.fori_loop(0, dst.shape[0], step, 0)

    blocks = BEAMS * rows
    half = blocks // 2
    halves = (pl.ds(0, half), pl.ds(half, half))
    opposite, straight = [], []
    for d in range(2):
        opposite.append(send_to(looked.at[across, halves[d]], opposite_half[d], col_ways[d]))
    for d in range(2):
        straight.append(
            send_to(
                looked.at[cols[d], halves[1 - d]], from_cols[d].at[halves[1 - d]], col_ways[d]
            )
        )
    step1 = [[] for _ in range(2)]
    for u in range(EARLY, count):
        for d in range(2):
            step1[d].append(send(late.at[u - EARLY], one[d].at[u - EARLY], d))
    step2 = [[send(scales1.at[d], two_s[d], d)] for d in range(2)]

    def forward(u):
        for d in range(2):
            if u < EARLY:
                src = items1.at[d * EARLY + u]
            else:
                step1[d][u - EARLY].wait_recv()
                src = one[d].at[u - EARLY]
            step2[d].append(send(src, two[d].at[u], d))

    forward(0)
    for d in range(2):
        opposite[d].wait()
        part = part_sum[d]
        add(part, opposite_half[d], looked.at[cols[d], halves[d]])
        straight.append(send_to(part, from_cols[d].at[halves[d]], col_ways[d]))
    for c in straight:
        c.wait_recv()
    add(col_sum, looked.at[col], from_cols[0], from_cols[1])
    row_sends = [
        send_to(col_sum.at[pl.ds(r * BEAMS, BEAMS)], from_rows[k], p)
        for k, (r, p) in enumerate(zip(row_ids, row_peers))
    ]
    for u in range(1, EARLY):
        forward(u)
    for c in row_sends:
        c.wait_recv()
    add(row_sum, col_sum.at[pl.ds(row * BEAMS, BEAMS)], *from_rows)
    reach = (BEAMS // 2, BEAMS // 2 - 1)
    passed = [[] for _ in range(2)]

    def pass_on():
        for d in range(2):
            k = len(passed[d])
            if k == reach[d]:
                continue
            distance = reach[d] - k
            block = BEAMS - distance if d == 0 else distance
            if k == 0:
                src = row_sum.at[block]
            else:
                passed[d][k - 1].wait_recv()
                hops[d][k] = row_sum[block] + from_beam[d][k - 1]
                src = hops[d].at[k]
            passed[d].append(send(src, from_beam[d].at[k], d))

    pass_on()
    for u in range(EARLY, count):
        forward(u)
        pass_on()
    step3 = []
    for d in range(2):
        for c in step2[d]:
            c.wait_recv()
        sign = 1 if d == 0 else -1
        origin = beam(-2 * sign)
        nearer = wanted_by(sign)
        farther = wanted_by(2 * sign)
        end = lowest if d == 0 else highest
        chosen = (
            lowest(nearer, origin, count), highest(nearer, origin, count), end(farther, origin, count)
        )
        for s in range(3):
            picked_s[d][s] = two_s[d][chosen[s]]
        for s in range(3):
            picked[d][s] = two[d][chosen[s]]
        step3.append([send(picked_s[d], three_s[d], d)])
        step3[d].append(send(picked[d].at[2], three[d].at[2], d))
    while any(len(passed[d]) < reach[d] for d in range(2)):
        pass_on()
    for d in range(2):
        step3[d].append(send(picked[d].at[0], three[d].at[0], d))
    step4 = []
    for d in range(2):
        step3[d][0].wait_recv()
        step4.append(send(three_s[d].at[2], four_s[d].at[0], d))
        step3[d][1].wait_recv()
        step4.append(send(three[d].at[2], four[d].at[0], d))
    for d in range(2):
        step3[d].append(send(picked[d].at[1], three[d].at[1], d))
    for d in range(2):
        passed[d][-1].wait_recv()
    entries[...] = (
        row_sum[0] + from_beam[0][reach[0] - 1] + from_beam[1][reach[1] - 1]
    ).astype(jnp.float32)
    for c in step4:
        c.wait_recv()
    for d in range(2):
        for c in step3[d][2:]:
            c.wait_recv()
    mine = wanted_by(0)
    for u in range(count):
        offset = (my_beam + BEAMS - mine(u)) % BEAMS
        third = [jnp.where(lowest(mine, beam(d), count) == u, 0, 1) for d in (-3, 3)]
        middle = lowest(mine, beam(4), count) == u
        rows_out = []
        for h in range(states.shape[1]):
            x = states[u, h]
            line = u * states.shape[1] + h

            def take(x, when, code, scale):
                return jnp.where(when, code.astype(jnp.int32).astype(jnp.float32) * scale, x)

            for d in range(2):
                near = items1[d * EARLY + u, h] if u < EARLY else one[d][u - EARLY, h]
                x = take(x, offset == (1, BEAMS - 1)[d], near, scales1[d, u, h : h + 1, :])
                x = take(
                    x, offset == (2, BEAMS - 2)[d], two[d][u, h], two_s[d][u, h : h + 1, :]
                )
                x = take(
                    x, offset == (3, BEAMS - 3)[d],
                    three[d][third[d], h], three_s[d][third[d], h : h + 1, :],
                )
                x = take(
                    x, (offset == 4) & (middle if d == 0 else jnp.logical_not(middle)),
                    four[d][0, h], four_s[d][0, h : h + 1, :],
                )
            state, out = advance(x, lambda k: entries[line : line + 1, k], gain[h : h + 1, :])
            new_states[u, h] = state
            rows_out.append(out)
        readout[u] = jnp.concatenate(rows_out, axis=0).astype(jnp.bfloat16)
    for c in copies:
        if id(c) not in set(map(id, opposite)):
            c.wait_send()


def relay(wants, states, items1, scales1, late, looked, gain):
    count, heads, size, _ = states.shape
    blocks, height, width = looked.shape[1:]
    rows = blocks // BEAMS
    sends = 2 * (1 + count) + 2 * (count - EARLY) + 2 * 4 + 4 + 6 + (rows - 1) + BEAMS - 1
    whole = pl.BlockSpec(memory_space=pltpu.VMEM)
    kept = [count, count, 3, 3, 1, 1, 3, 3]
    parts = [blocks // 2] * 2 + [blocks] * 2 + [BEAMS] * (rows - 1) + [blocks // 2] * 2
    parts += [BEAMS // 2] * 4 + [blocks, BEAMS]
    return pl.pallas_call(
        functools.partial(relay_kernel, count),
        out_shape=(
            jax.ShapeDtypeStruct((count, heads, size), jnp.bfloat16),
            jax.ShapeDtypeStruct(states.shape, jnp.float32),
        ),
        in_specs=[pl.BlockSpec(memory_space=pltpu.SMEM)] + [whole] * 6,
        out_specs=(whole, whole),
        scratch_shapes=[
            *(pltpu.VMEM((k, heads, size, size), jnp.int16) for k in kept),
            *(pltpu.VMEM((k, heads, size), jnp.float32) for k in kept),
            *(pltpu.VMEM((count - EARLY, heads, size, size), jnp.int16) for _ in range(2)),
            *(pltpu.VMEM((k, height, width), looked.dtype) for k in parts),
            pltpu.VMEM((height, width), jnp.float32),
            pltpu.SemaphoreType.DMA((sends,)),
            pltpu.SemaphoreType.DMA((sends,)),
        ],
        compiler_params=pltpu.CompilerParams(
            collective_id=1, has_side_effects=True, vmem_limit_bytes=40 << 20
        ),
    )(wants, states, items1, scales1, late, looked, gain)


def local(states, parent_beam, next_token, proj_table, gate_table, gain):
    count, heads, size, _ = states.shape
    devices = lax.axis_size("beam")
    spacing = devices // BEAMS
    position = lax.axis_index("beam")
    my_beam, within = position // spacing, position % spacing
    lanes = jnp.zeros((128,), jnp.int32)
    mine = jnp.concatenate([next_token, parent_beam])
    lanes = lax.dynamic_update_slice(lanes, mine, (within * 2 * count,))
    ids = jnp.broadcast_to(lanes[None, :], (8, 128))
    items1, scales1, table, late = gather(states, ids)
    every = table[:, 0, :].reshape(BEAMS, spacing, 2 * count)
    wants = lax.dynamic_slice_in_dim(every, within, 1, axis=1)[:, 0, count:]
    tokens = every[:, :, :count].reshape(BEAMS, spacing // ROW, ROW, count).transpose(2, 1, 0, 3).reshape(-1)

    vocab_rows = proj_table.shape[0]
    wide = 5 * size
    padded = jnp.concatenate(
        [
            proj_table.transpose(1, 0, 2),
            gate_table.transpose(2, 0, 1),
            jnp.zeros((heads, vocab_rows, size - 3), proj_table.dtype),
        ],
        axis=2,
    ).reshape(heads * vocab_rows, wide + size)
    wanted = jnp.repeat(tokens - position * vocab_rows, heads)
    head_at = jnp.arange(heads * vocab_rows, dtype=jnp.int32) // vocab_rows
    row_at = jnp.arange(heads * vocab_rows, dtype=jnp.int32) % vocab_rows
    own_head = jnp.arange(wanted.shape[0], dtype=jnp.int32) % heads
    onehot = (
        (wanted[:, None] == row_at[None, :]) & (own_head[:, None] == head_at[None, :])
    ).astype(jnp.bfloat16)
    looked = jnp.dot(onehot, padded, preferred_element_type=jnp.float32).astype(jnp.bfloat16)
    looked = looked.reshape(ROW, devices // ROW, count * heads, wide + size)
    return relay(wants, states, items1, scales1, late, looked, gain)


def solution(mesh):
    return jax.shard_map(
        local,
        mesh=mesh,
        in_specs=(
            P(("groups", "beam"), "mp", None, None),
            P(("groups", "beam")),
            P(("groups", "beam")),
            P("beam", "mp", None),
            P("beam", None, "mp"),
            P("mp", None),
        ),
        out_specs=(P(("groups", "beam"), "mp", None), P(("groups", "beam"), "mp", None, None)),
        check_vma=False,
    )
```

```python
import functools

import jax
import jax.numpy as jnp
from jax import lax
from jax.experimental import pallas as pl
from jax.experimental.pallas import tpu as pltpu
from jax.sharding import PartitionSpec as P

BEAMS = 8
ROW = 4
IDS = 8
LEVELS = 32767.0
EARLY = 2


def to(index):
    return dict(device_id={"beam": index}, device_id_type=pl.DeviceIdType.MESH)


def gather_kernel(count, states, ids, items, scales, table, late, q, qs, near, side, tile, sems, rsem):
    n = lax.axis_size("beam")
    me = lax.axis_index("beam")
    spacing = n // BEAMS
    rows = spacing // ROW
    my_beam, within = me // spacing, me % spacing
    row, col = within // ROW, within % ROW
    base = my_beam * spacing
    beam_peers = [(me + k * spacing) % n for k in range(1, BEAMS)]
    row_peers = [base + ((row + k) % rows) * ROW + col for k in range(1, rows)]
    col_peers = [base + row * ROW + (col + k) % ROW for k in range(1, ROW)]
    peers = beam_peers + row_peers + col_peers
    barrier = pltpu.get_barrier_semaphore()
    for p in peers:
        pl.semaphore_signal(barrier, inc=1, **to(p))
    pl.semaphore_wait(barrier, len(peers))

    copies = []
    at = [0]

    def send(src, dst, target):
        c = pltpu.make_async_remote_copy(
            src_ref=src, dst_ref=dst, send_sem=sems.at[at[0]], recv_sem=rsem.at[at[0]], **to(target)
        )
        at[0] += 1
        c.start()
        copies.append(c)
        return c

    def code(u):
        for h in range(states.shape[1]):
            x = states[u, h]
            top = jnp.maximum(jnp.max(jnp.abs(x), axis=0, keepdims=True), 1e-30)
            qs[u, h : h + 1, :] = top * (1.0 / LEVELS)
            code_to = q.at[u] if u < EARLY else late.at[u - EARLY]
            code_to[h] = lax.round(
                x * (LEVELS / top), lax.RoundingMethod.TO_NEAREST_EVEN
            ).astype(jnp.int32).astype(jnp.int16)

    first = [send(ids, near.at[k], p) for k, p in enumerate(row_peers)]
    code(0)
    ways = (beam_peers[0], beam_peers[-1])
    for d in range(2):
        send(q.at[0], items.at[d * EARLY], ways[d])
    for c in first:
        c.wait_recv()
    total = ids[...]
    for k in range(len(row_peers)):
        total = total + near[k]
    tile[0] = total
    for u in range(1, count):
        code(u)
    second = [send(tile.at[0], side.at[k], p) for k, p in enumerate(col_peers)]
    for c in second:
        c.wait_recv()
    for k in range(len(col_peers)):
        total = total + side[k]
    tile[1] = total
    for d in range(2):
        send(qs, scales.at[d], ways[d])
    for k, p in enumerate(beam_peers):
        send(tile.at[1], table.at[k + 1], p)
    for u in range(1, EARLY):
        for d in range(2):
            send(q.at[u], items.at[d * EARLY + u], ways[d])
    table[0] = total
    waited = set(map(id, first + second))
    for c in copies:
        c.wait_send()
        if id(c) not in waited:
            c.wait_recv()


def gather(states, ids):
    count, heads, size, _ = states.shape
    n = lax.axis_size("beam")
    rows = n // BEAMS // ROW
    sends = (rows - 1) + (ROW - 1) + (BEAMS - 1) + 2 * EARLY + 2
    whole = pl.BlockSpec(memory_space=pltpu.VMEM)
    return pl.pallas_call(
        functools.partial(gather_kernel, count),
        out_shape=(
            jax.ShapeDtypeStruct((2 * EARLY, heads, size, size), jnp.int16),
            jax.ShapeDtypeStruct((2, count, heads, size), jnp.float32),
            jax.ShapeDtypeStruct((BEAMS, 8, 128), jnp.int32),
            jax.ShapeDtypeStruct((count - EARLY, heads, size, size), jnp.int16),
        ),
        in_specs=[whole, whole],
        out_specs=(whole, whole, whole, whole),
        scratch_shapes=[
            pltpu.VMEM((EARLY, heads, size, size), jnp.int16),
            pltpu.VMEM((count, heads, size), jnp.float32),
            pltpu.VMEM((rows - 1, 8, 128), jnp.int32),
            pltpu.VMEM((ROW - 1, 8, 128), jnp.int32),
            pltpu.VMEM((2, 8, 128), jnp.int32),
            pltpu.SemaphoreType.DMA((sends,)),
            pltpu.SemaphoreType.DMA((sends,)),
        ],
        compiler_params=pltpu.CompilerParams(
            collective_id=0, has_side_effects=True, vmem_limit_bytes=24 << 20
        ),
    )(states, ids)


def lowest(row_of, beam, count):
    u = count - 1
    for k in range(count - 2, -1, -1):
        u = jnp.where(row_of(k) == beam, k, u)
    return u


def highest(row_of, beam, count):
    u = 0
    for k in range(1, count):
        u = jnp.where(row_of(k) == beam, k, u)
    return u


def advance(state, entry, gain):
    size = state.shape[0]
    eye = (
        lax.broadcasted_iota(jnp.int32, (size, size), 0)
        == lax.broadcasted_iota(jnp.int32, (size, size), 1)
    ).astype(jnp.float32)

    def vector(k):
        return entry(slice(k * size, (k + 1) * size))

    def unit(x):
        return x * lax.rsqrt(jnp.sum(x * x, axis=-1, keepdims=True) + 1e-06)

    def gate(k):
        x = entry(slice(5 * size + k, 5 * size + k + 1))
        return 1.0 / (1.0 + jnp.exp(-jnp.broadcast_to(x, (1, size))))

    state = gate(0) * state
    for j in range(2):
        key = unit(vector(1 + j))
        gap = jnp.sum(state * key - eye * vector(3 + j), axis=-1, keepdims=True)
        state = state - gap * (2.0 * gate(1 + j) * key)
    out = jnp.sum(state * unit(vector(0)), axis=-1, keepdims=True)
    row = jnp.sum(eye * out, axis=0, keepdims=True)
    scale = lax.rsqrt(jnp.sum(row * row, axis=-1, keepdims=True) * (1.0 / size) + 1e-05)
    return state, gain * row * scale


def relay_kernel(
    count, wants, states, items1, scales1, late, looked, gain, readout, new_states, *scratch
):
    two, three, four, picked = scratch[0:2], scratch[2:4], scratch[4:6], scratch[6:8]
    two_s, three_s, four_s, picked_s = scratch[8:10], scratch[10:12], scratch[12:14], scratch[14:16]
    one = scratch[16:18]
    opposite_half, from_cols, part_sum = scratch[18:20], scratch[20:22], scratch[22:24]
    hops, from_row = scratch[24:26], scratch[26:28]
    col_sum, entries, sems, rsem = scratch[28:]
    n = lax.axis_size("beam")
    me = lax.axis_index("beam")
    spacing = n // BEAMS
    my_beam = me // spacing
    rows = spacing // ROW
    within = me % spacing
    row, col = within // ROW, within % ROW
    base = my_beam * spacing
    ways = ((me + spacing) % n, (me + n - spacing) % n)
    cols = ((col + 1) % ROW, (col + ROW - 1) % ROW)
    across = (col + 2) % ROW
    col_ways = [base + row * ROW + c for c in cols]
    row_ways = ((me + ROW) % n, (me + n - ROW) % n)
    barrier = pltpu.get_barrier_semaphore()
    peers = [*ways, *col_ways, *row_ways]
    for p in peers:
        pl.semaphore_signal(barrier, inc=1, **to(p))
    pl.semaphore_wait(barrier, len(peers))

    def beam(d):
        return (my_beam + BEAMS + d) % BEAMS

    def wanted_by(d):
        return lambda u: wants[(BEAMS - d) % BEAMS, u]

    copies = []
    at = [0]

    def send_to(src, dst, target):
        c = pltpu.make_async_remote_copy(
            src_ref=src, dst_ref=dst, send_sem=sems.at[at[0]], recv_sem=rsem.at[at[0]], **to(target)
        )
        at[0] += 1
        c.start()
        copies.append(c)
        return c

    def send(src, dst, way):
        return send_to(src, dst, ways[way])

    def add(dst, *srcs):
        def step(i, _):
            x = srcs[0][i]
            for y in srcs[1:]:
                x = x + y[i]
            dst[i] = x
            return 0

        lax.fori_loop(0, dst.shape[0], step, 0)

    blocks = BEAMS * rows
    half = blocks // 2
    halves = (pl.ds(0, half), pl.ds(half, half))
    opposite, straight = [], []
    for d in range(2):
        opposite.append(send_to(looked.at[across, halves[d]], opposite_half[d], col_ways[d]))
    for d in range(2):
        straight.append(
            send_to(
                looked.at[cols[d], halves[1 - d]], from_cols[d].at[halves[1 - d]], col_ways[d]
            )
        )
    heads = states.shape[1]
    step1 = [{}, {}]
    step2 = [{}, {}]
    step3 = [{}, {}]
    step4 = [{}, {}]

    def send1(u, h):
        for d in range(2):
            step1[d][u, h] = send(late.at[u - EARLY, h], one[d].at[u - EARLY, h], d)

    def send2(u, h):
        for d in range(2):
            if u < EARLY:
                src = items1.at[d * EARLY + u, h]
            else:
                step1[d][u, h].wait_recv()
                src = one[d].at[u - EARLY, h]
            step2[d][u, h] = send(src, two[d].at[u, h], d)

    def pick():
        for d in range(2):
            for c in step2[d].values():
                c.wait_recv()
            sign = 1 if d == 0 else -1
            origin = beam(-2 * sign)
            nearer = wanted_by(sign)
            farther = wanted_by(2 * sign)
            end = lowest if d == 0 else highest
            chosen = (
                lowest(nearer, origin, count),
                highest(nearer, origin, count),
                end(farther, origin, count),
            )
            for s in (2, 0, 1):
                picked_s[d][s] = two_s[d][chosen[s]]
                picked[d][s] = two[d][chosen[s]]
            step3[d]["scales"] = send(picked_s[d], three_s[d], d)

    def send3(s, h):
        for d in range(2):
            step3[d][s, h] = send(picked[d].at[s, h], three[d].at[s, h], d)

    def send4(h):
        for d in range(2):
            if h == 0:
                step3[d]["scales"].wait_recv()
                step4[d]["scales"] = send(three_s[d].at[2], four_s[d].at[0], d)
            step3[d][2, h].wait_recv()
            step4[d][h] = send(three[d].at[2, h], four[d].at[0, h], d)

    each = range(heads)
    todo = [functools.partial(send1, u, h) for u in range(EARLY, count) for h in each]
    todo += [functools.partial(send2, 0, h) for h in each]
    ahead = len(todo)
    todo += [functools.partial(send2, u, h) for u in range(1, count) for h in each]
    todo += [functools.partial(send3, s, h) for s in (2, 0) for h in each]
    picking = todo[len(todo) - 2 * heads]
    todo += [functools.partial(send4, h) for h in each]
    todo += [functools.partial(send3, 1, h) for h in each]
    for d in range(2):
        step2[d]["scales"] = send(scales1.at[d], two_s[d], d)
    for unit in todo[:ahead]:
        unit()
    for d in range(2):
        opposite[d].wait()
        part = part_sum[d]
        add(part, opposite_half[d], looked.at[cols[d], halves[d]])
        straight.append(send_to(part, from_cols[d].at[halves[d]], col_ways[d]))
    for c in straight:
        c.wait_recv()
    add(col_sum, looked.at[col], from_cols[0], from_cols[1])

    reach = (blocks // 2, blocks // 2 - 1)
    passed = [[] for _ in range(2)]

    def block(distance):
        z = (my_beam * rows + row + blocks + distance) % blocks
        return (z % rows) * BEAMS + (my_beam + BEAMS - z // rows) % BEAMS

    def pass_on():
        for d in range(2):
            k = len(passed[d])
            if k == reach[d]:
                continue
            at_block = block(reach[d] - k if d == 0 else k - reach[d])
            if k == 0:
                src = col_sum.at[at_block]
            else:
                passed[d][k - 1].wait_recv()
                hops[d][k] = col_sum[at_block] + from_row[d][k - 1]
                src = hops[d].at[k]
            passed[d].append(send_to(src, from_row[d].at[k], row_ways[d]))

    rest = todo[ahead:]
    pass_on()
    for i, unit in enumerate(rest):
        if unit is picking:
            pick()
        unit()
        while len(passed[0]) < min(reach[0], 1 + (i + 1) * reach[0] // len(rest)):
            pass_on()
    for d in range(2):
        passed[d][-1].wait_recv()
    entries[...] = (
        col_sum[block(0)] + from_row[0][reach[0] - 1] + from_row[1][reach[1] - 1]
    ).astype(jnp.float32)
    for d in range(2):
        for key, c in step3[d].items():
            if key != "scales" and key[0] != 2:
                c.wait_recv()
        for c in step4[d].values():
            c.wait_recv()
    mine = wanted_by(0)
    for u in range(count):
        offset = (my_beam + BEAMS - mine(u)) % BEAMS
        third = [jnp.where(lowest(mine, beam(d), count) == u, 0, 1) for d in (-3, 3)]
        middle = lowest(mine, beam(4), count) == u
        rows_out = []
        for h in range(states.shape[1]):
            x = states[u, h]
            line = u * states.shape[1] + h

            def take(x, when, code, scale):
                return jnp.where(when, code.astype(jnp.int32).astype(jnp.float32) * scale, x)

            for d in range(2):
                near = items1[d * EARLY + u, h] if u < EARLY else one[d][u - EARLY, h]
                x = take(x, offset == (1, BEAMS - 1)[d], near, scales1[d, u, h : h + 1, :])
                x = take(
                    x, offset == (2, BEAMS - 2)[d], two[d][u, h], two_s[d][u, h : h + 1, :]
                )
                x = take(
                    x, offset == (3, BEAMS - 3)[d],
                    three[d][third[d], h], three_s[d][third[d], h : h + 1, :],
                )
                x = take(
                    x, (offset == 4) & (middle if d == 0 else jnp.logical_not(middle)),
                    four[d][0, h], four_s[d][0, h : h + 1, :],
                )
            state, out = advance(x, lambda k: entries[line : line + 1, k], gain[h : h + 1, :])
            new_states[u, h] = state
            rows_out.append(out)
        readout[u] = jnp.concatenate(rows_out, axis=0).astype(jnp.bfloat16)
    for c in copies:
        if id(c) not in set(map(id, opposite)):
            c.wait_send()


def relay(wants, states, items1, scales1, late, looked, gain):
    count, heads, size, _ = states.shape
    blocks, height, width = looked.shape[1:]
    sends = 2 * heads * (count - EARLY + count + 4) + 2 * 3 + 6 + blocks - 1
    whole = pl.BlockSpec(memory_space=pltpu.VMEM)
    kept = [count, count, 3, 3, 1, 1, 3, 3]
    parts = [blocks // 2] * 2 + [blocks] * 2 + [blocks // 2] * 6 + [blocks]
    return pl.pallas_call(
        functools.partial(relay_kernel, count),
        out_shape=(
            jax.ShapeDtypeStruct((count, heads, size), jnp.bfloat16),
            jax.ShapeDtypeStruct(states.shape, jnp.float32),
        ),
        in_specs=[pl.BlockSpec(memory_space=pltpu.SMEM)] + [whole] * 6,
        out_specs=(whole, whole),
        scratch_shapes=[
            *(pltpu.VMEM((k, heads, size, size), jnp.int16) for k in kept),
            *(pltpu.VMEM((k, heads, size), jnp.float32) for k in kept),
            *(pltpu.VMEM((count - EARLY, heads, size, size), jnp.int16) for _ in range(2)),
            *(pltpu.VMEM((k, height, width), looked.dtype) for k in parts),
            pltpu.VMEM((height, width), jnp.float32),
            pltpu.SemaphoreType.DMA((sends,)),
            pltpu.SemaphoreType.DMA((sends,)),
        ],
        compiler_params=pltpu.CompilerParams(
            collective_id=1, has_side_effects=True, vmem_limit_bytes=40 << 20
        ),
    )(wants, states, items1, scales1, late, looked, gain)


def local(states, parent_beam, next_token, proj_table, gate_table, gain):
    count, heads, size, _ = states.shape
    devices = lax.axis_size("beam")
    spacing = devices // BEAMS
    position = lax.axis_index("beam")
    my_beam, within = position // spacing, position % spacing
    lanes = jnp.zeros((128,), jnp.int32)
    mine = jnp.concatenate([next_token, parent_beam])
    lanes = lax.dynamic_update_slice(lanes, mine, (within * 2 * count,))
    ids = jnp.broadcast_to(lanes[None, :], (8, 128))
    items1, scales1, table, late = gather(states, ids)
    every = table[:, 0, :].reshape(BEAMS, spacing, 2 * count)
    wants = lax.dynamic_slice_in_dim(every, within, 1, axis=1)[:, 0, count:]
    tokens = every[:, :, :count].reshape(BEAMS, spacing // ROW, ROW, count).transpose(2, 1, 0, 3).reshape(-1)

    vocab_rows = proj_table.shape[0]
    wide = 5 * size
    padded = jnp.concatenate(
        [
            proj_table.transpose(1, 0, 2),
            gate_table.transpose(2, 0, 1),
            jnp.zeros((heads, vocab_rows, size - 3), proj_table.dtype),
        ],
        axis=2,
    ).reshape(heads * vocab_rows, wide + size)
    wanted = jnp.repeat(tokens - position * vocab_rows, heads)
    head_at = jnp.arange(heads * vocab_rows, dtype=jnp.int32) // vocab_rows
    row_at = jnp.arange(heads * vocab_rows, dtype=jnp.int32) % vocab_rows
    own_head = jnp.arange(wanted.shape[0], dtype=jnp.int32) % heads
    onehot = (
        (wanted[:, None] == row_at[None, :]) & (own_head[:, None] == head_at[None, :])
    ).astype(jnp.bfloat16)
    looked = jnp.dot(onehot, padded, preferred_element_type=jnp.float32).astype(jnp.bfloat16)
    looked = looked.reshape(ROW, devices // ROW, count * heads, wide + size)
    return relay(wants, states, items1, scales1, late, looked, gain)


def solution(mesh):
    return jax.shard_map(
        local,
        mesh=mesh,
        in_specs=(
            P(("groups", "beam"), "mp", None, None),
            P(("groups", "beam")),
            P(("groups", "beam")),
            P("beam", "mp", None),
            P("beam", None, "mp"),
            P("mp", None),
        ),
        out_specs=(P(("groups", "beam"), "mp", None), P(("groups", "beam"), "mp", None, None)),
        check_vma=False,
    )
```

```python
import functools

import jax
import jax.numpy as jnp
from jax import lax
from jax.experimental import pallas as pl
from jax.experimental.pallas import tpu as pltpu
from jax.sharding import PartitionSpec as P

BEAMS = 8
ROW = 4
IDS = 8
LEVELS = 32767.0


def to(index):
    return dict(device_id={"beam": index}, device_id_type=pl.DeviceIdType.MESH)


def lowest(row_of, beam, count):
    u = count - 1
    for k in range(count - 2, -1, -1):
        u = jnp.where(row_of(k) == beam, k, u)
    return u


def highest(row_of, beam, count):
    u = 0
    for k in range(1, count):
        u = jnp.where(row_of(k) == beam, k, u)
    return u


def advance(state, entry, gain):
    size = state.shape[0]
    eye = (
        lax.broadcasted_iota(jnp.int32, (size, size), 0)
        == lax.broadcasted_iota(jnp.int32, (size, size), 1)
    ).astype(jnp.float32)

    def vector(k):
        return entry(slice(k * size, (k + 1) * size))

    def unit(x):
        return x * lax.rsqrt(jnp.sum(x * x, axis=-1, keepdims=True) + 1e-06)

    def gate(k):
        x = entry(slice(5 * size + k, 5 * size + k + 1))
        return 1.0 / (1.0 + jnp.exp(-jnp.broadcast_to(x, (1, size))))

    state = gate(0) * state
    for j in range(2):
        key = unit(vector(1 + j))
        gap = jnp.sum(state * key - eye * vector(3 + j), axis=-1, keepdims=True)
        state = state - gap * (2.0 * gate(1 + j) * key)
    out = jnp.sum(state * unit(vector(0)), axis=-1, keepdims=True)
    row = jnp.sum(eye * out, axis=0, keepdims=True)
    scale = lax.rsqrt(jnp.sum(row * row, axis=-1, keepdims=True) * (1.0 / size) + 1e-05)
    return state, gain * row * scale


def step_kernel(count, states, ids, rows_of_tokens, gain, readout, new_states, *scratch):
    two, three, four, picked = scratch[0:2], scratch[2:4], scratch[4:6], scratch[6:8]
    two_s, three_s, four_s, picked_s = scratch[8:10], scratch[10:12], scratch[12:14], scratch[14:16]
    one, one_s = scratch[16:18], scratch[18:20]
    opposite_half, from_cols, part_sum = scratch[20:22], scratch[22:24], scratch[24:26]
    hops, from_row = scratch[26:28], scratch[28:30]
    col_sum, entries, looked, q, qs, near, side, tile, table, wants, copied, sems, rsem = scratch[30:]
    n = lax.axis_size("beam")
    me = lax.axis_index("beam")
    spacing = n // BEAMS
    my_beam = me // spacing
    rows = spacing // ROW
    within = me % spacing
    row, col = within // ROW, within % ROW
    base = my_beam * spacing
    ways = ((me + spacing) % n, (me + n - spacing) % n)
    cols = ((col + 1) % ROW, (col + ROW - 1) % ROW)
    across = (col + 2) % ROW
    col_ways = [base + row * ROW + c for c in cols]
    row_ways = ((me + ROW) % n, (me + n - ROW) % n)
    barrier = pltpu.get_barrier_semaphore()
    beam_peers = [(me + k * spacing) % n for k in range(1, BEAMS)]
    row_peers = [base + ((row + k) % rows) * ROW + col for k in range(1, rows)]
    col_peers = [base + row * ROW + (col + k) % ROW for k in range(1, ROW)]
    peers = [*beam_peers, *row_peers, *col_peers, *row_ways]
    for p in peers:
        pl.semaphore_signal(barrier, inc=1, **to(p))
    pl.semaphore_wait(barrier, len(peers))

    def beam(d):
        return (my_beam + BEAMS + d) % BEAMS

    def wanted_by(d):
        return lambda u: wants[(BEAMS - d) % BEAMS, 2, within * count + u]

    copies = []
    at = [0]

    def send_to(src, dst, target):
        c = pltpu.make_async_remote_copy(
            src_ref=src, dst_ref=dst, send_sem=sems.at[at[0]], recv_sem=rsem.at[at[0]], **to(target)
        )
        at[0] += 1
        c.start()
        copies.append(c)
        return c

    def send(src, dst, way):
        return send_to(src, dst, ways[way])

    def add(dst, *srcs):
        def step(i, _):
            x = srcs[0][i]
            for y in srcs[1:]:
                x = x + y[i]
            dst[i] = x
            return 0

        lax.fori_loop(0, dst.shape[0], step, 0)

    blocks = BEAMS * rows
    half = blocks // 2
    halves = (pl.ds(0, half), pl.ds(half, half))

    def code(u):
        for h in range(states.shape[1]):
            x = states[u, h]
            top = jnp.maximum(jnp.max(jnp.abs(x), axis=0, keepdims=True), 1e-30)
            qs[u, h : h + 1, :] = top * (1.0 / LEVELS)
            q[u, h] = lax.round(
                x * (LEVELS / top), lax.RoundingMethod.TO_NEAREST_EVEN
            ).astype(jnp.int32).astype(jnp.int16)

    def look_up():
        lines = rows_of_tokens.shape[0]
        heads = states.shape[1]
        vocab_rows = lines // heads
        lanes = tile.shape[-1]
        per = count * heads
        head = lax.rem(lax.broadcasted_iota(jnp.int32, (1, lanes), 1), heads)
        at_line = lax.broadcasted_iota(jnp.int32, (lines, lanes), 0)
        for k in range(BEAMS):
            for r in range(spacing * per // lanes):
                token = table[k, r : r + 1, :] - me * vocab_rows
                mine = (token >= 0) & (token < vocab_rows)
                line = jnp.where(mine, token + head * vocab_rows, -1)
                onehot = jnp.where(at_line == line, 1.0, 0.0).astype(jnp.bfloat16)
                out = lax.dot_general(
                    onehot, rows_of_tokens[...], (((0,), (0,)), ((), ())),
                    preferred_element_type=jnp.float32,
                ).astype(looked.dtype)
                for w in range(lanes // per):
                    dev = r * (lanes // per) + w
                    looked[dev % ROW, (dev // ROW) * BEAMS + k] = out[w * per : (w + 1) * per, :]

    heads = states.shape[1]
    step1 = [{}, {}]
    step2 = [{}, {}]
    step3 = [{}, {}]
    step4 = [{}, {}]

    def send1(u, h):
        for d in range(2):
            step1[d][u, h] = send(q.at[u, h], one[d].at[u, h], d)

    def send2(u, h):
        for d in range(2):
            step1[d][u, h].wait_recv()
            step2[d][u, h] = send(one[d].at[u, h], two[d].at[u, h], d)

    def pick():
        for d in range(2):
            for c in step2[d].values():
                c.wait_recv()
            sign = 1 if d == 0 else -1
            origin = beam(-2 * sign)
            nearer = wanted_by(sign)
            farther = wanted_by(2 * sign)
            end = lowest if d == 0 else highest
            chosen = (
                lowest(nearer, origin, count),
                highest(nearer, origin, count),
                end(farther, origin, count),
            )
            for s in (2, 0, 1):
                picked_s[d][s] = two_s[d][chosen[s]]
                picked[d][s] = two[d][chosen[s]]
            step3[d]["scales"] = send(picked_s[d], three_s[d], d)

    def send3(s, h):
        for d in range(2):
            step3[d][s, h] = send(picked[d].at[s, h], three[d].at[s, h], d)

    def send4(h):
        for d in range(2):
            if h == 0:
                step3[d]["scales"].wait_recv()
                step4[d]["scales"] = send(three_s[d].at[2], four_s[d].at[0], d)
            step3[d][2, h].wait_recv()
            step4[d][h] = send(three[d].at[2, h], four[d].at[0, h], d)

    each = range(heads)
    first = [send_to(ids, near.at[k], p) for k, p in enumerate(row_peers)]
    code(0)
    for h in each:
        send1(0, h)
    for u in range(1, count):
        code(u)
    for c in first:
        c.wait_recv()
    total = ids[...]
    for k in range(len(row_peers)):
        total = total + near[k]
    tile[0] = total
    first = [send_to(tile.at[0], side.at[k], p) for k, p in enumerate(col_peers)]
    for c in first:
        c.wait_recv()
    for k in range(len(col_peers)):
        total = total + side[k]
    tile[1] = total
    table[0] = total
    first = [send_to(tile.at[1], table.at[k + 1], p) for k, p in enumerate(beam_peers)]
    for d in range(2):
        step1[d]["scales"] = send(qs, one_s[d], d)
    for u in range(1, count - 1):
        for h in each:
            send1(u, h)
    for c in first:
        c.wait_recv()
    to_scalars = pltpu.make_async_copy(table, wants, copied)
    to_scalars.start()
    look_up()
    to_scalars.wait()
    opposite, straight = [], []
    for d in range(2):
        opposite.append(send_to(looked.at[across, halves[d]], opposite_half[d], col_ways[d]))
    for d in range(2):
        straight.append(
            send_to(
                looked.at[cols[d], halves[1 - d]], from_cols[d].at[halves[1 - d]], col_ways[d]
            )
        )
    for d in range(2):
        step1[d]["scales"].wait_recv()
        step2[d]["scales"] = send(one_s[d], two_s[d], d)
    for h in each:
        send1(count - 1, h)
    for h in each:
        send2(0, h)
    todo = [functools.partial(send2, u, h) for u in range(1, count) for h in each]
    todo += [functools.partial(send3, s, h) for s in (2, 0) for h in each]
    picking = todo[len(todo) - 2 * heads]
    todo += [functools.partial(send4, h) for h in each]
    todo += [functools.partial(send3, 1, h) for h in each]
    for d in range(2):
        opposite[d].wait()
        part = part_sum[d]
        add(part, opposite_half[d], looked.at[cols[d], halves[d]])
        straight.append(send_to(part, from_cols[d].at[halves[d]], col_ways[d]))
    for c in straight:
        c.wait_recv()
    add(col_sum, looked.at[col], from_cols[0], from_cols[1])

    reach = (blocks // 2, blocks // 2 - 1)
    passed = [[] for _ in range(2)]

    def block(distance):
        z = (my_beam * rows + row + blocks + distance) % blocks
        return (z % rows) * BEAMS + (my_beam + BEAMS - z // rows) % BEAMS

    def pass_on():
        for d in range(2):
            k = len(passed[d])
            if k == reach[d]:
                continue
            at_block = block(reach[d] - k if d == 0 else k - reach[d])
            if k == 0:
                src = col_sum.at[at_block]
            else:
                passed[d][k - 1].wait_recv()
                hops[d][k] = col_sum[at_block] + from_row[d][k - 1]
                src = hops[d].at[k]
            passed[d].append(send_to(src, from_row[d].at[k], row_ways[d]))

    pass_on()
    for i, unit in enumerate(todo):
        if unit is picking:
            pick()
        unit()
        while len(passed[0]) < min(reach[0], 1 + (i + 1) * reach[0] // len(todo)):
            pass_on()
    for d in range(2):
        passed[d][-1].wait_recv()
    entries[...] = (
        col_sum[block(0)] + from_row[0][reach[0] - 1] + from_row[1][reach[1] - 1]
    ).astype(jnp.float32)
    for d in range(2):
        for key, c in step3[d].items():
            if key != "scales" and key[0] != 2:
                c.wait_recv()
        for c in step4[d].values():
            c.wait_recv()
    mine = wanted_by(0)
    for u in range(count):
        offset = (my_beam + BEAMS - mine(u)) % BEAMS
        third = [jnp.where(lowest(mine, beam(d), count) == u, 0, 1) for d in (-3, 3)]
        middle = lowest(mine, beam(4), count) == u
        rows_out = []
        for h in range(states.shape[1]):
            x = states[u, h]
            line = u * states.shape[1] + h

            def take(x, when, code, scale):
                return jnp.where(when, code.astype(jnp.int32).astype(jnp.float32) * scale, x)

            for d in range(2):
                x = take(
                    x, offset == (1, BEAMS - 1)[d], one[d][u, h], one_s[d][u, h : h + 1, :]
                )
                x = take(
                    x, offset == (2, BEAMS - 2)[d], two[d][u, h], two_s[d][u, h : h + 1, :]
                )
                x = take(
                    x, offset == (3, BEAMS - 3)[d],
                    three[d][third[d], h], three_s[d][third[d], h : h + 1, :],
                )
                x = take(
                    x, (offset == 4) & (middle if d == 0 else jnp.logical_not(middle)),
                    four[d][0, h], four_s[d][0, h : h + 1, :],
                )
            state, out = advance(x, lambda k: entries[line : line + 1, k], gain[h : h + 1, :])
            new_states[u, h] = state
            rows_out.append(out)
        readout[u] = jnp.concatenate(rows_out, axis=0).astype(jnp.bfloat16)
    for c in copies:
        if id(c) not in set(map(id, opposite)):
            c.wait_send()


def step(states, ids, rows_of_tokens, gain):
    count, heads, size, _ = states.shape
    blocks = lax.axis_size("beam") // ROW
    rows = blocks // BEAMS
    height, width = count * heads, rows_of_tokens.shape[1]
    sends = 2 * heads * (2 * count + 4) + 2 * 4 + 6 + blocks - 1 + (rows - 1) + (ROW - 1) + BEAMS - 1
    whole = pl.BlockSpec(memory_space=pltpu.VMEM)
    kept = [count, count, 3, 3, 1, 1, 3, 3]
    parts = [blocks // 2] * 2 + [blocks] * 2 + [blocks // 2] * 6 + [blocks]
    kind = rows_of_tokens.dtype
    codes, floats, block = jnp.int16, jnp.float32, (height, width)
    return pl.pallas_call(
        functools.partial(step_kernel, count),
        out_shape=(
            jax.ShapeDtypeStruct((count, heads, size), jnp.bfloat16),
            jax.ShapeDtypeStruct(states.shape, floats),
        ),
        in_specs=[whole] * 4,
        out_specs=(whole, whole),
        scratch_shapes=[
            *(pltpu.VMEM((k, heads, size, size), codes) for k in kept),
            *(pltpu.VMEM((k, heads, size), floats) for k in kept),
            *(pltpu.VMEM((count, heads, size, size), codes) for _ in range(2)),
            *(pltpu.VMEM((count, heads, size), floats) for _ in range(2)),
            *(pltpu.VMEM((k, *block), kind) for k in parts),
            pltpu.VMEM(block, floats),
            pltpu.VMEM((ROW, blocks, *block), kind),
            pltpu.VMEM((count, heads, size, size), codes),
            pltpu.VMEM((count, heads, size), floats),
            pltpu.VMEM((rows - 1, *ids.shape), jnp.int32),
            pltpu.VMEM((ROW - 1, *ids.shape), jnp.int32),
            pltpu.VMEM((2, *ids.shape), jnp.int32),
            pltpu.VMEM((BEAMS, *ids.shape), jnp.int32),
            pltpu.SMEM((BEAMS, *ids.shape), jnp.int32),
            pltpu.SemaphoreType.DMA,
            pltpu.SemaphoreType.DMA((sends,)),
            pltpu.SemaphoreType.DMA((sends,)),
        ],
        compiler_params=pltpu.CompilerParams(
            collective_id=0, has_side_effects=True, vmem_limit_bytes=48 << 20
        ),
    )(states, ids, rows_of_tokens, gain)


def local(states, parent_beam, next_token, proj_table, gate_table, gain):
    count, heads, size, _ = states.shape
    spacing = lax.axis_size("beam") // BEAMS
    within = lax.axis_index("beam") % spacing
    lanes = 128
    given = jnp.zeros((8 * lanes,), jnp.int32)
    given = lax.dynamic_update_slice(
        given, jnp.repeat(next_token, heads), (within * count * heads,)
    )
    given = lax.dynamic_update_slice(given, parent_beam, (2 * lanes + within * count,))
    vocab_rows = proj_table.shape[0]
    padded = jnp.concatenate(
        [
            proj_table.transpose(1, 0, 2),
            gate_table.transpose(2, 0, 1),
            jnp.zeros((heads, vocab_rows, size - 3), proj_table.dtype),
        ],
        axis=2,
    ).reshape(heads * vocab_rows, 6 * size)
    return step(states, given.reshape(8, lanes), padded, gain)


def solution(mesh):
    return jax.shard_map(
        local,
        mesh=mesh,
        in_specs=(
            P(("groups", "beam"), "mp", None, None),
            P(("groups", "beam")),
            P(("groups", "beam")),
            P("beam", "mp", None),
            P("beam", None, "mp"),
            P("mp", None),
        ),
        out_specs=(P(("groups", "beam"), "mp", None), P(("groups", "beam"), "mp", None, None)),
        check_vma=False,
    )
```

```python
import functools

import jax
import jax.numpy as jnp
from jax import lax
from jax.experimental import pallas as pl
from jax.experimental.pallas import tpu as pltpu
from jax.sharding import PartitionSpec as P

BEAMS = 8
ROW = 4
IDS = 8
LEVELS = 32767.0


def to(index):
    return dict(device_id={"beam": index}, device_id_type=pl.DeviceIdType.MESH)


def lowest(row_of, beam, count):
    u = count - 1
    for k in range(count - 2, -1, -1):
        u = jnp.where(row_of(k) == beam, k, u)
    return u


def highest(row_of, beam, count):
    u = 0
    for k in range(1, count):
        u = jnp.where(row_of(k) == beam, k, u)
    return u


def advance(state, entry, gain):
    size = state.shape[0]
    eye = (
        lax.broadcasted_iota(jnp.int32, (size, size), 0)
        == lax.broadcasted_iota(jnp.int32, (size, size), 1)
    ).astype(jnp.float32)

    def vector(k):
        return entry(slice(k * size, (k + 1) * size))

    def unit(x):
        return x * lax.rsqrt(jnp.sum(x * x, axis=-1, keepdims=True) + 1e-06)

    def gate(k):
        x = entry(slice(5 * size + k, 5 * size + k + 1))
        return 1.0 / (1.0 + jnp.exp(-jnp.broadcast_to(x, (1, size))))

    state = gate(0) * state
    for j in range(2):
        key = unit(vector(1 + j))
        gap = jnp.sum(state * key - eye * vector(3 + j), axis=-1, keepdims=True)
        state = state - gap * (2.0 * gate(1 + j) * key)
    out = jnp.sum(state * unit(vector(0)), axis=-1, keepdims=True)
    row = jnp.sum(eye * out, axis=0, keepdims=True)
    scale = lax.rsqrt(jnp.sum(row * row, axis=-1, keepdims=True) * (1.0 / size) + 1e-05)
    return state, gain * row * scale


def step_kernel(count, states, ids, rows_of_tokens, gain, readout, new_states, *scratch):
    heads = states.shape[1]
    refs = iter(scratch)

    def take_refs(k):
        return [next(refs) for _ in range(k)]

    two, three, four, picked = ([take_refs(heads) for _ in range(2)] for _ in range(4))
    two_s, three_s, four_s, picked_s, one, one_s = (take_refs(2) for _ in range(6))
    opposite_half, from_cols, part_sum, hops, from_row = (take_refs(2) for _ in range(5))
    col_sum, entries, looked, q, qs, near, side, tile, table, wants, copied, sems, rsem = refs
    n = lax.axis_size("beam")
    me = lax.axis_index("beam")
    spacing = n // BEAMS
    my_beam = me // spacing
    rows = spacing // ROW
    within = me % spacing
    row, col = within // ROW, within % ROW
    base = my_beam * spacing
    ways = ((me + spacing) % n, (me + n - spacing) % n)
    cols = ((col + 1) % ROW, (col + ROW - 1) % ROW)
    across = (col + 2) % ROW
    col_ways = [base + row * ROW + c for c in cols]
    row_ways = ((me + ROW) % n, (me + n - ROW) % n)
    barrier = pltpu.get_barrier_semaphore()
    beam_peers = [(me + k * spacing) % n for k in range(1, BEAMS)]
    row_peers = [base + ((row + k) % rows) * ROW + col for k in range(1, rows)]
    col_peers = [base + row * ROW + (col + k) % ROW for k in range(1, ROW)]
    peers = [*beam_peers, *row_peers, *col_peers, *row_ways]
    for p in peers:
        pl.semaphore_signal(barrier, inc=1, **to(p))
    pl.semaphore_wait(barrier, len(peers))

    def beam(d):
        return (my_beam + BEAMS + d) % BEAMS

    def wanted_by(d):
        return lambda u: wants[(BEAMS - d) % BEAMS, 2, within * count + u]

    copies = []
    at = [0]

    def send_to(src, dst, target):
        c = pltpu.make_async_remote_copy(
            src_ref=src, dst_ref=dst, send_sem=sems.at[at[0]], recv_sem=rsem.at[at[0]], **to(target)
        )
        at[0] += 1
        c.start()
        copies.append(c)
        return c

    def send(src, dst, way):
        return send_to(src, dst, ways[way])

    def add(dst, *srcs):
        def step(i, _):
            x = srcs[0][i]
            for y in srcs[1:]:
                x = x + y[i]
            dst[i] = x
            return 0

        lax.fori_loop(0, dst.shape[0], step, 0)

    blocks = BEAMS * rows
    half = blocks // 2
    halves = (pl.ds(0, half), pl.ds(half, half))

    def code(h):
        for u in range(count):
            x = states[u, h]
            top = jnp.maximum(jnp.max(jnp.abs(x), axis=0, keepdims=True), 1e-30)
            qs[u, h : h + 1, :] = top * (1.0 / LEVELS)
            q[u, h] = lax.round(
                x * (LEVELS / top), lax.RoundingMethod.TO_NEAREST_EVEN
            ).astype(jnp.int32).astype(jnp.int16)

    def look_up():
        lines = rows_of_tokens.shape[0]
        vocab_rows = lines // heads
        lanes = tile.shape[-1]
        per = count * heads
        head = lax.rem(lax.broadcasted_iota(jnp.int32, (1, lanes), 1), heads)
        at_line = lax.broadcasted_iota(jnp.int32, (lines, lanes), 0)
        for k in range(BEAMS):
            for r in range(spacing * per // lanes):
                token = table[k, r : r + 1, :] - me * vocab_rows
                mine = (token >= 0) & (token < vocab_rows)
                line = jnp.where(mine, token + head * vocab_rows, -1)
                onehot = jnp.where(at_line == line, 1.0, 0.0).astype(jnp.bfloat16)
                out = lax.dot_general(
                    onehot, rows_of_tokens[...], (((0,), (0,)), ((), ())),
                    preferred_element_type=jnp.float32,
                ).astype(looked.dtype)
                for w in range(lanes // per):
                    dev = r * (lanes // per) + w
                    looked[dev % ROW, (dev // ROW) * BEAMS + k] = out[w * per : (w + 1) * per, :]

    step1 = [{}, {}]
    step2 = [{}, {}]
    step3 = [{}, {}]
    step4 = [{}, {}]

    def send1(u, h):
        for d in range(2):
            step1[d][u, h] = send(q.at[u, h], one[d].at[u, h], d)

    def send2(u, h):
        for d in range(2):
            step1[d][u, h].wait_recv()
            step2[d][u, h] = send(one[d].at[u, h], two[d][h].at[u], d)

    def choice(d):
        sign = 1 if d == 0 else -1
        origin = beam(-2 * sign)
        nearer = wanted_by(sign)
        end = lowest if d == 0 else highest
        return (
            lowest(nearer, origin, count),
            highest(nearer, origin, count),
            end(wanted_by(2 * sign), origin, count),
        )

    def pick(h, chosen):
        for d in range(2):
            if h == 0:
                step2[d]["scales"].wait_recv()
                for s in range(3):
                    picked_s[d][s] = two_s[d][chosen[d][s]]
                step3[d]["scales"] = send(picked_s[d], three_s[d], d)
            for u in range(count):
                step2[d][u, h].wait_recv()
            for s in range(3):
                picked[d][h][s] = two[d][h][chosen[d][s]]

    def send3(s, h, chosen):
        if s == 2:
            pick(h, chosen)
        for d in range(2):
            step3[d][s, h] = send(picked[d][h].at[s], three[d][h].at[s], d)

    def send4(h):
        for d in range(2):
            if h == 0:
                step3[d]["scales"].wait_recv()
                step4[d]["scales"] = send(three_s[d].at[2], four_s[d].at[0], d)
            step3[d][2, h].wait_recv()
            step4[d][h] = send(three[d][h].at[2], four[d][h].at[0], d)

    each = range(heads)
    first = [send_to(ids, near.at[k], p) for k, p in enumerate(row_peers)]
    every = range(count)
    code(0)
    for u in every:
        send1(u, 0)
    for h in each[1:]:
        code(h)
    for c in first:
        c.wait_recv()
    total = ids[...]
    for k in range(len(row_peers)):
        total = total + near[k]
    tile[0] = total
    first = [send_to(tile.at[0], side.at[k], p) for k, p in enumerate(col_peers)]
    for c in first:
        c.wait_recv()
    for k in range(len(col_peers)):
        total = total + side[k]
    tile[1] = total
    table[0] = total
    first = [send_to(tile.at[1], table.at[k + 1], p) for k, p in enumerate(beam_peers)]
    for d in range(2):
        step1[d]["scales"] = send(qs, one_s[d], d)
    for h in each[1:-1]:
        for u in every:
            send1(u, h)
    for c in first:
        c.wait_recv()
    to_scalars = pltpu.make_async_copy(table, wants, copied)
    to_scalars.start()
    look_up()
    to_scalars.wait()
    opposite, straight = [], []
    for d in range(2):
        opposite.append(send_to(looked.at[across, halves[d]], opposite_half[d], col_ways[d]))
    for d in range(2):
        straight.append(
            send_to(
                looked.at[cols[d], halves[1 - d]], from_cols[d].at[halves[1 - d]], col_ways[d]
            )
        )
    for d in range(2):
        step1[d]["scales"].wait_recv()
        step2[d]["scales"] = send(one_s[d], two_s[d], d)
    for u in every:
        send1(u, heads - 1)
    for u in every:
        send2(u, 0)
    todo = [functools.partial(send2, u, h) for h in each[1:] for u in every]
    chosen = [choice(d) for d in range(2)]
    for h in each:
        todo.append(functools.partial(send3, 2, h, chosen))
        if h > 0:
            todo.append(functools.partial(send4, h - 1))
        todo.append(functools.partial(send3, 0, h, chosen))
        if h == heads - 1:
            todo.append(functools.partial(send4, h))
        todo.append(functools.partial(send3, 1, h, chosen))
    for d in range(2):
        opposite[d].wait()
        part = part_sum[d]
        add(part, opposite_half[d], looked.at[cols[d], halves[d]])
        straight.append(send_to(part, from_cols[d].at[halves[d]], col_ways[d]))
    for c in straight:
        c.wait_recv()
    add(col_sum, looked.at[col], from_cols[0], from_cols[1])

    reach = (blocks // 2, blocks // 2 - 1)
    passed = [[] for _ in range(2)]

    def block(distance):
        z = (my_beam * rows + row + blocks + distance) % blocks
        return (z % rows) * BEAMS + (my_beam + BEAMS - z // rows) % BEAMS

    def pass_on():
        for d in range(2):
            k = len(passed[d])
            if k == reach[d]:
                continue
            at_block = block(reach[d] - k if d == 0 else k - reach[d])
            if k == 0:
                src = col_sum.at[at_block]
            else:
                passed[d][k - 1].wait_recv()
                hops[d][k] = col_sum[at_block] + from_row[d][k - 1]
                src = hops[d].at[k]
            passed[d].append(send_to(src, from_row[d].at[k], row_ways[d]))

    pass_on()
    for i, unit in enumerate(todo):
        unit()
        while len(passed[0]) < min(reach[0], 1 + (i + 1) * reach[0] // len(todo)):
            pass_on()
    for d in range(2):
        passed[d][-1].wait_recv()
    entries[...] = (
        col_sum[block(0)] + from_row[0][reach[0] - 1] + from_row[1][reach[1] - 1]
    ).astype(jnp.float32)
    for d in range(2):
        step4[d]["scales"].wait_recv()
    mine = wanted_by(0)
    offsets = [(my_beam + BEAMS - mine(u)) % BEAMS for u in every]
    third = [[jnp.where(lowest(mine, beam(b), count) == u, 0, 1) for b in (-3, 3)] for u in every]
    across_first = lowest(mine, beam(4), count)

    def take(x, when, code, scale):
        return jnp.where(when, code.astype(jnp.int32).astype(jnp.float32) * scale, x)

    outs = [[] for _ in every]
    for h in each:
        for d in range(2):
            step3[d][0, h].wait_recv()
            step3[d][1, h].wait_recv()
            step4[d][h].wait_recv()
        at_h = slice(h, h + 1)
        for u in every:
            x = states[u, h]
            offset = offsets[u]
            middle = across_first == u
            for d in range(2):
                t = third[u][d]
                x = take(x, offset == (1, BEAMS - 1)[d], one[d][u, h], one_s[d][u, at_h, :])
                x = take(x, offset == (2, BEAMS - 2)[d], two[d][h][u], two_s[d][u, at_h, :])
                x = take(x, offset == (3, BEAMS - 3)[d], three[d][h][t], three_s[d][t, at_h, :])
                x = take(
                    x, (offset == 4) & (middle if d == 0 else jnp.logical_not(middle)),
                    four[d][h][0], four_s[d][0, at_h, :],
                )
            line = u * heads + h
            state, out = advance(x, lambda k: entries[line : line + 1, k], gain[at_h, :])
            new_states[u, h] = state
            outs[u].append(out)
    for u in every:
        readout[u] = jnp.concatenate(outs[u], axis=0).astype(jnp.bfloat16)
    for c in copies:
        if id(c) not in set(map(id, opposite)):
            c.wait_send()


def step(states, ids, rows_of_tokens, gain):
    count, heads, size, _ = states.shape
    blocks = lax.axis_size("beam") // ROW
    rows = blocks // BEAMS
    height, width = count * heads, rows_of_tokens.shape[1]
    sends = 2 * heads * (2 * count + 4) + 2 * 4 + 6 + blocks - 1 + (rows - 1) + (ROW - 1) + BEAMS - 1
    whole = pl.BlockSpec(memory_space=pltpu.VMEM)
    kept = [count, count, 3, 3, 1, 1, 3, 3]
    parts = [blocks // 2] * 2 + [blocks] * 2 + [blocks // 2] * 6 + [blocks]
    kind = rows_of_tokens.dtype
    codes, floats, block = jnp.int16, jnp.float32, (height, width)
    return pl.pallas_call(
        functools.partial(step_kernel, count),
        out_shape=(
            jax.ShapeDtypeStruct((count, heads, size), jnp.bfloat16),
            jax.ShapeDtypeStruct(states.shape, floats),
        ),
        in_specs=[whole] * 4,
        out_specs=(whole, whole),
        scratch_shapes=[
            *(pltpu.VMEM((k, size, size), codes) for k in kept for _ in range(heads)),
            *(pltpu.VMEM((k, heads, size), floats) for k in kept),
            *(pltpu.VMEM((count, heads, size, size), codes) for _ in range(2)),
            *(pltpu.VMEM((count, heads, size), floats) for _ in range(2)),
            *(pltpu.VMEM((k, *block), kind) for k in parts),
            pltpu.VMEM(block, floats),
            pltpu.VMEM((ROW, blocks, *block), kind),
            pltpu.VMEM((count, heads, size, size), codes),
            pltpu.VMEM((count, heads, size), floats),
            pltpu.VMEM((rows - 1, *ids.shape), jnp.int32),
            pltpu.VMEM((ROW - 1, *ids.shape), jnp.int32),
            pltpu.VMEM((2, *ids.shape), jnp.int32),
            pltpu.VMEM((BEAMS, *ids.shape), jnp.int32),
            pltpu.SMEM((BEAMS, *ids.shape), jnp.int32),
            pltpu.SemaphoreType.DMA,
            pltpu.SemaphoreType.DMA((sends,)),
            pltpu.SemaphoreType.DMA((sends,)),
        ],
        compiler_params=pltpu.CompilerParams(
            collective_id=0, has_side_effects=True, vmem_limit_bytes=48 << 20
        ),
    )(states, ids, rows_of_tokens, gain)


def local(states, parent_beam, next_token, proj_table, gate_table, gain):
    count, heads, size, _ = states.shape
    spacing = lax.axis_size("beam") // BEAMS
    within = lax.axis_index("beam") % spacing
    lanes = 128
    given = jnp.zeros((8 * lanes,), jnp.int32)
    given = lax.dynamic_update_slice(
        given, jnp.repeat(next_token, heads), (within * count * heads,)
    )
    given = lax.dynamic_update_slice(given, parent_beam, (2 * lanes + within * count,))
    vocab_rows = proj_table.shape[0]
    padded = jnp.concatenate(
        [
            proj_table.transpose(1, 0, 2),
            gate_table.transpose(2, 0, 1),
            jnp.zeros((heads, vocab_rows, size - 3), proj_table.dtype),
        ],
        axis=2,
    ).reshape(heads * vocab_rows, 6 * size)
    return step(states, given.reshape(8, lanes), padded, gain)


def solution(mesh):
    return jax.shard_map(
        local,
        mesh=mesh,
        in_specs=(
            P(("groups", "beam"), "mp", None, None),
            P(("groups", "beam")),
            P(("groups", "beam")),
            P("beam", "mp", None),
            P("beam", None, "mp"),
            P("mp", None),
        ),
        out_specs=(P(("groups", "beam"), "mp", None), P(("groups", "beam"), "mp", None, None)),
        check_vma=False,
    )
```

```python
import functools

import jax
import jax.numpy as jnp
from jax import lax
from jax.experimental import pallas as pl
from jax.experimental.pallas import tpu as pltpu
from jax.sharding import PartitionSpec as P

BEAMS = 8
ROW = 4
IDS = 8
LEVELS = 32767.0


def to(index):
    return dict(device_id={"beam": index}, device_id_type=pl.DeviceIdType.MESH)


def lowest(row_of, beam, count):
    u = count - 1
    for k in range(count - 2, -1, -1):
        u = jnp.where(row_of(k) == beam, k, u)
    return u


def highest(row_of, beam, count):
    u = 0
    for k in range(1, count):
        u = jnp.where(row_of(k) == beam, k, u)
    return u


def advance(state, entry, gain):
    size = state.shape[0]
    eye = (
        lax.broadcasted_iota(jnp.int32, (size, size), 0)
        == lax.broadcasted_iota(jnp.int32, (size, size), 1)
    ).astype(jnp.float32)

    def vector(k):
        return entry(slice(k * size, (k + 1) * size))

    def unit(x):
        return x * lax.rsqrt(jnp.sum(x * x, axis=-1, keepdims=True) + 1e-06)

    def gate(k):
        x = entry(slice(5 * size + k, 5 * size + k + 1))
        return 1.0 / (1.0 + jnp.exp(-jnp.broadcast_to(x, (1, size))))

    state = gate(0) * state
    for j in range(2):
        key = unit(vector(1 + j))
        gap = jnp.sum(state * key - eye * vector(3 + j), axis=-1, keepdims=True)
        state = state - gap * (2.0 * gate(1 + j) * key)
    out = jnp.sum(state * unit(vector(0)), axis=-1, keepdims=True)
    row = jnp.sum(eye * out, axis=0, keepdims=True)
    scale = lax.rsqrt(jnp.sum(row * row, axis=-1, keepdims=True) * (1.0 / size) + 1e-05)
    return state, gain * row * scale


def step_kernel(
    count, tokens, parents, states_in, rows_of_tokens, gain, readout, new_states, *scratch
):
    heads, size = states_in.shape[1], states_in.shape[2]
    refs = iter(scratch)

    def take_refs(k):
        return [next(refs) for _ in range(k)]

    two, three, four, picked = ([take_refs(heads) for _ in range(2)] for _ in range(4))
    two_s, three_s, four_s, picked_s, one, one_s = (take_refs(2) for _ in range(6))
    opposite_half, from_cols, part_sum, hops, from_row = (take_refs(2) for _ in range(5))
    col_sum, entries, looked, states, q, qs, ids, near, side, tile, table, wants = take_refs(12)
    copied, fetched, ready, sems, rsem = refs
    fetch = pltpu.make_async_copy(states_in, states, fetched)
    fetch.start()
    n = lax.axis_size("beam")
    me = lax.axis_index("beam")
    spacing = n // BEAMS
    my_beam = me // spacing
    rows = spacing // ROW
    within = me % spacing
    row, col = within // ROW, within % ROW
    base = my_beam * spacing
    ways = ((me + spacing) % n, (me + n - spacing) % n)
    cols = ((col + 1) % ROW, (col + ROW - 1) % ROW)
    across = (col + 2) % ROW
    col_ways = [base + row * ROW + c for c in cols]
    row_ways = ((me + ROW) % n, (me + n - ROW) % n)
    barrier = pltpu.get_barrier_semaphore()
    beam_peers = [(me + k * spacing) % n for k in range(1, BEAMS)]
    row_peers = [base + ((row + k) % rows) * ROW + col for k in range(1, rows)]
    col_peers = [base + row * ROW + (col + k) % ROW for k in range(1, ROW)]
    peers = [*ways, *row_peers, *col_peers, *row_ways]
    for p in peers:
        pl.semaphore_signal(barrier, inc=1, **to(p))
    pl.semaphore_wait(barrier, len(peers))

    def beam(d):
        return (my_beam + BEAMS + d) % BEAMS

    def wanted_by(d):
        return lambda u: wants[(BEAMS - d) % BEAMS, 2, within * count + u]

    copies = []
    at = [0]

    def send_to(src, dst, target):
        c = pltpu.make_async_remote_copy(
            src_ref=src, dst_ref=dst, send_sem=sems.at[at[0]], recv_sem=rsem.at[at[0]], **to(target)
        )
        at[0] += 1
        c.start()
        copies.append(c)
        return c

    def send(src, dst, way):
        return send_to(src, dst, ways[way])

    def add(dst, *srcs):
        def step(i, _):
            x = srcs[0][i]
            for y in srcs[1:]:
                x = x + y[i]
            dst[i] = x
            return 0

        lax.fori_loop(0, dst.shape[0], step, 0)

    blocks = BEAMS * rows
    half = blocks // 2
    halves = (pl.ds(0, half), pl.ds(half, half))

    def code(h):
        for u in range(count):
            x = states[u, h]
            top = jnp.maximum(jnp.max(jnp.abs(x), axis=0, keepdims=True), 1e-30)
            qs[u, h : h + 1, :] = top * (1.0 / LEVELS)
            q[u, h] = lax.round(
                x * (LEVELS / top), lax.RoundingMethod.TO_NEAREST_EVEN
            ).astype(jnp.int32).astype(jnp.int16)

    def look_up():
        lines = rows_of_tokens.shape[0]
        vocab_rows = lines // heads
        lanes = tile.shape[-1]
        per = count * heads
        head = lax.rem(lax.broadcasted_iota(jnp.int32, (1, lanes), 1), heads)
        at_line = lax.broadcasted_iota(jnp.int32, (lines, lanes), 0)
        for k in range(BEAMS):
            for r in range(spacing * per // lanes):
                token = table[k, r : r + 1, :] - me * vocab_rows
                mine = (token >= 0) & (token < vocab_rows)
                line = jnp.where(mine, token + head * vocab_rows, -1)
                onehot = jnp.where(at_line == line, 1.0, 0.0).astype(jnp.bfloat16)
                out = lax.dot_general(
                    onehot, rows_of_tokens[...], (((0,), (0,)), ((), ())),
                    preferred_element_type=jnp.float32,
                ).astype(looked.dtype)
                for w in range(lanes // per):
                    dev = r * (lanes // per) + w
                    looked[dev % ROW, (dev // ROW) * BEAMS + k] = out[w * per : (w + 1) * per, :]

    step1 = [{}, {}]
    step2 = [{}, {}]
    step3 = [{}, {}]
    step4 = [{}, {}]

    def send1(u, h):
        for d in range(2):
            step1[d][u, h] = send(q.at[u, h], one[d].at[u, h], d)

    def send2(u, h):
        for d in range(2):
            step1[d][u, h].wait_recv()
            step2[d][u, h] = send(one[d].at[u, h], two[d][h].at[u], d)

    def choice(d):
        sign = 1 if d == 0 else -1
        origin = beam(-2 * sign)
        nearer = wanted_by(sign)
        end = lowest if d == 0 else highest
        return (
            lowest(nearer, origin, count),
            highest(nearer, origin, count),
            end(wanted_by(2 * sign), origin, count),
        )

    def pick(h, chosen):
        for d in range(2):
            if h == 0:
                step2[d]["scales"].wait_recv()
                for s in range(3):
                    picked_s[d][s] = two_s[d][chosen[d][s]]
                step3[d]["scales"] = send(picked_s[d], three_s[d], d)
            for u in range(count):
                step2[d][u, h].wait_recv()
            for s in range(3):
                picked[d][h][s] = two[d][h][chosen[d][s]]

    def send3(s, h, chosen):
        if s == 2:
            pick(h, chosen)
        for d in range(2):
            step3[d][s, h] = send(picked[d][h].at[s], three[d][h].at[s], d)

    def send4(h):
        for d in range(2):
            if h == 0:
                step3[d]["scales"].wait_recv()
                step4[d]["scales"] = send(three_s[d].at[2], four_s[d].at[0], d)
            step3[d][2, h].wait_recv()
            step4[d][h] = send(three[d][h].at[2], four[d][h].at[0], d)

    each = range(heads)
    def announce(j):
        for d in range(2):
            pl.semaphore_signal(ready.at[d, j], inc=1, **to(ways[d]))

    def hear(j):
        for d in range(2):
            pl.semaphore_wait(ready.at[d, j], 1)

    lanes = ids.shape[1]
    spot = lax.broadcasted_iota(jnp.int32, ids.shape, 0) * lanes
    spot = spot + lax.broadcasted_iota(jnp.int32, ids.shape, 1)
    own = jnp.zeros(ids.shape, jnp.int32)
    for u in range(count):
        start = (within * count + u) * heads
        own = jnp.where((spot >= start) & (spot < start + heads), tokens[u], own)
        own = jnp.where(spot == 2 * lanes + within * count + u, parents[u], own)
    ids[...] = own
    every = range(count)
    announce(0)
    first = [send_to(ids, near.at[k], p) for k, p in enumerate(row_peers)]
    fetch.wait()
    code(0)
    for u in every:
        send1(u, 0)
    hear(0)
    announce(1)
    for h in each[1:]:
        code(h)
    for c in first:
        c.wait_recv()
    total = ids[...]
    for k in range(len(row_peers)):
        total = total + near[k]
    tile[0] = total
    first = [send_to(tile.at[0], side.at[k], p) for k, p in enumerate(col_peers)]
    hear(1)
    announce(2)
    for c in first:
        c.wait_recv()
    for k in range(len(col_peers)):
        total = total + side[k]
    tile[1] = total
    table[0] = total
    hear(2)
    first = [send_to(tile.at[1], table.at[k + 1], p) for k, p in enumerate(beam_peers)]
    for d in range(2):
        step1[d]["scales"] = send(qs, one_s[d], d)
    for h in each[1:-1]:
        for u in every:
            send1(u, h)
    for c in first:
        c.wait_recv()
    to_scalars = pltpu.make_async_copy(table, wants, copied)
    to_scalars.start()
    look_up()
    to_scalars.wait()
    opposite, straight = [], []
    for d in range(2):
        opposite.append(send_to(looked.at[across, halves[d]], opposite_half[d], col_ways[d]))
    for d in range(2):
        straight.append(
            send_to(
                looked.at[cols[d], halves[1 - d]], from_cols[d].at[halves[1 - d]], col_ways[d]
            )
        )
    for d in range(2):
        step1[d]["scales"].wait_recv()
        step2[d]["scales"] = send(one_s[d], two_s[d], d)
    for u in every:
        send1(u, heads - 1)
    for u in every:
        send2(u, 0)
    todo = [functools.partial(send2, u, h) for h in each[1:] for u in every]
    chosen = [choice(d) for d in range(2)]
    for h in each:
        todo.append(functools.partial(send3, 2, h, chosen))
        if h > 0:
            todo.append(functools.partial(send4, h - 1))
        todo.append(functools.partial(send3, 0, h, chosen))
        if h == heads - 1:
            todo.append(functools.partial(send4, h))
        todo.append(functools.partial(send3, 1, h, chosen))
    for d in range(2):
        opposite[d].wait()
        part = part_sum[d]
        add(part, opposite_half[d], looked.at[cols[d], halves[d]])
        straight.append(send_to(part, from_cols[d].at[halves[d]], col_ways[d]))
    for c in straight:
        c.wait_recv()
    add(col_sum, looked.at[col], from_cols[0], from_cols[1])

    reach = (blocks // 2, blocks // 2 - 1)
    passed = [[] for _ in range(2)]

    def block(distance):
        z = (my_beam * rows + row + blocks + distance) % blocks
        return (z % rows) * BEAMS + (my_beam + BEAMS - z // rows) % BEAMS

    def pass_on():
        for d in range(2):
            k = len(passed[d])
            if k == reach[d]:
                continue
            at_block = block(reach[d] - k if d == 0 else k - reach[d])
            if k == 0:
                src = col_sum.at[at_block]
            else:
                passed[d][k - 1].wait_recv()
                hops[d][k] = col_sum[at_block] + from_row[d][k - 1]
                src = hops[d].at[k]
            passed[d].append(send_to(src, from_row[d].at[k], row_ways[d]))

    pass_on()
    for i, unit in enumerate(todo):
        unit()
        while len(passed[0]) < min(reach[0], 1 + (i + 1) * reach[0] // len(todo)):
            pass_on()
    for d in range(2):
        passed[d][-1].wait_recv()
    entries[...] = (
        col_sum[block(0)] + from_row[0][reach[0] - 1] + from_row[1][reach[1] - 1]
    ).astype(jnp.float32)
    for d in range(2):
        step4[d]["scales"].wait_recv()
    mine = wanted_by(0)
    offsets = [(my_beam + BEAMS - mine(u)) % BEAMS for u in every]
    third = [[jnp.where(lowest(mine, beam(b), count) == u, 0, 1) for b in (-3, 3)] for u in every]
    across_first = lowest(mine, beam(4), count)

    def take(x, when, code, scale):
        return jnp.where(when, code.astype(jnp.int32).astype(jnp.float32) * scale, x)

    outs = [[] for _ in every]
    for h in each:
        for d in range(2):
            step3[d][0, h].wait_recv()
            step3[d][1, h].wait_recv()
            step4[d][h].wait_recv()
        at_h = slice(h, h + 1)
        for u in every:
            x = states[u, h]
            offset = offsets[u]
            middle = across_first == u
            for d in range(2):
                t = third[u][d]
                x = take(x, offset == (1, BEAMS - 1)[d], one[d][u, h], one_s[d][u, at_h, :])
                x = take(x, offset == (2, BEAMS - 2)[d], two[d][h][u], two_s[d][u, at_h, :])
                x = take(x, offset == (3, BEAMS - 3)[d], three[d][h][t], three_s[d][t, at_h, :])
                x = take(
                    x, (offset == 4) & (middle if d == 0 else jnp.logical_not(middle)),
                    four[d][h][0], four_s[d][0, at_h, :],
                )
            line = u * heads + h
            state, out = advance(x, lambda k: entries[line : line + 1, k], gain[at_h, :])
            new_states[u, h] = state
            outs[u].append(out)
    for u in every:
        readout[u] = jnp.concatenate(outs[u], axis=0).astype(jnp.bfloat16)
    for c in copies:
        if id(c) not in set(map(id, opposite)):
            c.wait_send()


def step(tokens, parents, states, rows_of_tokens, gain):
    count, heads, size, _ = states.shape
    blocks = lax.axis_size("beam") // ROW
    rows = blocks // BEAMS
    height, width = count * heads, rows_of_tokens.shape[1]
    sends = 2 * heads * (2 * count + 4) + 2 * 4 + 6 + blocks - 1 + (rows - 1) + (ROW - 1) + BEAMS - 1
    whole = pl.BlockSpec(memory_space=pltpu.VMEM)
    kept = [count, count, 3, 3, 1, 1, 3, 3]
    parts = [blocks // 2] * 2 + [blocks] * 2 + [blocks // 2] * 6 + [blocks]
    kind = rows_of_tokens.dtype
    codes, floats, block, ids = jnp.int16, jnp.float32, (height, width), (8, 128)
    scalars = pl.BlockSpec(memory_space=pltpu.SMEM)
    return pl.pallas_call(
        functools.partial(step_kernel, count),
        out_shape=(
            jax.ShapeDtypeStruct((count, heads, size), jnp.bfloat16),
            jax.ShapeDtypeStruct(states.shape, floats),
        ),
        in_specs=[scalars, scalars, pl.BlockSpec(memory_space=pltpu.HBM), whole, whole],
        out_specs=(whole, whole),
        scratch_shapes=[
            *(pltpu.VMEM((k, size, size), codes) for k in kept for _ in range(heads)),
            *(pltpu.VMEM((k, heads, size), floats) for k in kept),
            *(pltpu.VMEM((count, heads, size, size), codes) for _ in range(2)),
            *(pltpu.VMEM((count, heads, size), floats) for _ in range(2)),
            *(pltpu.VMEM((k, *block), kind) for k in parts),
            pltpu.VMEM(block, floats),
            pltpu.VMEM((ROW, blocks, *block), kind),
            pltpu.VMEM(states.shape, floats),
            pltpu.VMEM(states.shape, codes),
            pltpu.VMEM((count, heads, size), floats),
            pltpu.VMEM(ids, jnp.int32),
            pltpu.VMEM((rows - 1, *ids), jnp.int32),
            pltpu.VMEM((ROW - 1, *ids), jnp.int32),
            pltpu.VMEM((2, *ids), jnp.int32),
            pltpu.VMEM((BEAMS, *ids), jnp.int32),
            pltpu.SMEM((BEAMS, *ids), jnp.int32),
            pltpu.SemaphoreType.DMA,
            pltpu.SemaphoreType.DMA,
            pltpu.SemaphoreType.REGULAR((2, BEAMS // 2 - 1)),
            pltpu.SemaphoreType.DMA((sends,)),
            pltpu.SemaphoreType.DMA((sends,)),
        ],
        compiler_params=pltpu.CompilerParams(
            collective_id=0, has_side_effects=True, vmem_limit_bytes=48 << 20
        ),
    )(tokens, parents, states, rows_of_tokens, gain)


def local(states, parent_beam, next_token, proj_table, gate_table, gain):
    heads, size = states.shape[1:3]
    vocab_rows = proj_table.shape[0]
    padded = jnp.concatenate(
        [
            proj_table.transpose(1, 0, 2),
            gate_table.transpose(2, 0, 1),
            jnp.zeros((heads, vocab_rows, size - 3), proj_table.dtype),
        ],
        axis=2,
    ).reshape(heads * vocab_rows, 6 * size)
    return step(next_token, parent_beam, states, padded, gain)


def solution(mesh):
    return jax.shard_map(
        local,
        mesh=mesh,
        in_specs=(
            P(("groups", "beam"), "mp", None, None),
            P(("groups", "beam")),
            P(("groups", "beam")),
            P("beam", "mp", None),
            P("beam", None, "mp"),
            P("mp", None),
        ),
        out_specs=(P(("groups", "beam"), "mp", None), P(("groups", "beam"), "mp", None, None)),
        check_vma=False,
    )
```

```python
import functools

import jax
import jax.numpy as jnp
from jax import lax
from jax.experimental import pallas as pl
from jax.experimental.pallas import tpu as pltpu
from jax.sharding import PartitionSpec as P

BEAMS = 8
ROW = 4
IDS = 8
LEVELS = 32767.0


def to(index):
    return dict(device_id={"beam": index}, device_id_type=pl.DeviceIdType.MESH)


def lowest(row_of, beam, count):
    u = count - 1
    for k in range(count - 2, -1, -1):
        u = jnp.where(row_of(k) == beam, k, u)
    return u


def highest(row_of, beam, count):
    u = 0
    for k in range(1, count):
        u = jnp.where(row_of(k) == beam, k, u)
    return u


def advance(state, entry, gain):
    size = state.shape[0]
    eye = (
        lax.broadcasted_iota(jnp.int32, (size, size), 0)
        == lax.broadcasted_iota(jnp.int32, (size, size), 1)
    ).astype(jnp.float32)

    def vector(k):
        return entry(slice(k * size, (k + 1) * size))

    def unit(x):
        return x * lax.rsqrt(jnp.sum(x * x, axis=-1, keepdims=True) + 1e-06)

    def gate(k):
        x = entry(slice(5 * size + k, 5 * size + k + 1))
        return 1.0 / (1.0 + jnp.exp(-jnp.broadcast_to(x, (1, size))))

    state = gate(0) * state
    for j in range(2):
        key = unit(vector(1 + j))
        gap = jnp.sum(state * key - eye * vector(3 + j), axis=-1, keepdims=True)
        state = state - gap * (2.0 * gate(1 + j) * key)
    out = jnp.sum(state * unit(vector(0)), axis=-1, keepdims=True)
    row = jnp.sum(eye * out, axis=0, keepdims=True)
    scale = lax.rsqrt(jnp.sum(row * row, axis=-1, keepdims=True) * (1.0 / size) + 1e-05)
    return state, gain * row * scale


def step_kernel(
    count, tokens, parents, states_in, rows_of_tokens, gain, readout, new_states, *scratch
):
    heads, size = states_in.shape[1], states_in.shape[2]
    refs = iter(scratch)

    def take_refs(k):
        return [next(refs) for _ in range(k)]

    two, three, four, picked = ([take_refs(heads) for _ in range(2)] for _ in range(4))
    two_s, three_s, four_s, picked_s, one, one_s = (take_refs(2) for _ in range(6))
    opposite_half, from_cols, part_sum, hops, from_row, from_pair = (take_refs(2) for _ in range(6))
    pair_sum = next(refs)
    col_sum, entries, looked, states, q, qs, ids, near, side, tile, table, wants = take_refs(12)
    copied, fetched, ready, sems, rsem = refs
    fetch = pltpu.make_async_copy(states_in, states, fetched)
    fetch.start()
    n = lax.axis_size("beam")
    me = lax.axis_index("beam")
    spacing = n // BEAMS
    my_beam = me // spacing
    rows = spacing // ROW
    within = me % spacing
    row, col = within // ROW, within % ROW
    base = my_beam * spacing
    ways = ((me + spacing) % n, (me + n - spacing) % n)
    cols = ((col + 1) % ROW, (col + ROW - 1) % ROW)
    across = (col + 2) % ROW
    col_ways = [base + row * ROW + c for c in cols]
    row_ways = ((me + 2 * ROW) % n, (me + n - 2 * ROW) % n)
    parity = row % 2
    partner = base + (row + 1 - 2 * parity) * ROW + col
    barrier = pltpu.get_barrier_semaphore()
    beam_peers = [(me + k * spacing) % n for k in range(1, BEAMS)]
    row_peers = [base + ((row + k) % rows) * ROW + col for k in range(1, rows)]
    col_peers = [base + row * ROW + (col + k) % ROW for k in range(1, ROW)]
    peers = [*ways, *row_peers, *col_peers, *row_ways]
    for p in peers:
        pl.semaphore_signal(barrier, inc=1, **to(p))
    pl.semaphore_wait(barrier, len(peers))

    def beam(d):
        return (my_beam + BEAMS + d) % BEAMS

    def wanted_by(d):
        return lambda u: wants[(BEAMS - d) % BEAMS, 2, within * count + u]

    copies = []
    at = [0]

    def send_to(src, dst, target):
        c = pltpu.make_async_remote_copy(
            src_ref=src, dst_ref=dst, send_sem=sems.at[at[0]], recv_sem=rsem.at[at[0]], **to(target)
        )
        at[0] += 1
        c.start()
        copies.append(c)
        return c

    def send(src, dst, way):
        return send_to(src, dst, ways[way])

    def add(dst, *srcs):
        def step(i, _):
            x = srcs[0][i]
            for y in srcs[1:]:
                x = x + y[i]
            dst[i] = x
            return 0

        lax.fori_loop(0, dst.shape[0], step, 0)

    blocks = BEAMS * rows
    half = blocks // 2
    halves = (pl.ds(0, half), pl.ds(half, half))

    def code(h):
        for u in range(count):
            x = states[u, h]
            top = jnp.maximum(jnp.max(jnp.abs(x), axis=0, keepdims=True), 1e-30)
            qs[u, h : h + 1, :] = top * (1.0 / LEVELS)
            q[u, h] = lax.round(
                x * (LEVELS / top), lax.RoundingMethod.TO_NEAREST_EVEN
            ).astype(jnp.int32).astype(jnp.int16)

    def look_up():
        lines = rows_of_tokens.shape[0]
        vocab_rows = lines // heads
        lanes = tile.shape[-1]
        per = count * heads
        head = lax.rem(lax.broadcasted_iota(jnp.int32, (1, lanes), 1), heads)
        at_line = lax.broadcasted_iota(jnp.int32, (lines, lanes), 0)
        for k in range(BEAMS):
            for r in range(spacing * per // lanes):
                token = table[k, r : r + 1, :] - me * vocab_rows
                mine = (token >= 0) & (token < vocab_rows)
                line = jnp.where(mine, token + head * vocab_rows, -1)
                onehot = jnp.where(at_line == line, 1.0, 0.0).astype(jnp.bfloat16)
                out = lax.dot_general(
                    onehot, rows_of_tokens[...], (((0,), (0,)), ((), ())),
                    preferred_element_type=jnp.float32,
                ).astype(looked.dtype)
                for w in range(lanes // per):
                    dev = r * (lanes // per) + w
                    looked[dev % ROW, (dev // ROW) * BEAMS + k] = out[w * per : (w + 1) * per, :]

    step1 = [{}, {}]
    step2 = [{}, {}]
    step3 = [{}, {}]
    step4 = [{}, {}]

    def send1(u, h):
        for d in range(2):
            step1[d][u, h] = send(q.at[u, h], one[d].at[u, h], d)

    def send2(u, h):
        for d in range(2):
            step1[d][u, h].wait_recv()
            step2[d][u, h] = send(one[d].at[u, h], two[d][h].at[u], d)

    def choice(d):
        sign = 1 if d == 0 else -1
        origin = beam(-2 * sign)
        nearer = wanted_by(sign)
        end = lowest if d == 0 else highest
        return (
            lowest(nearer, origin, count),
            highest(nearer, origin, count),
            end(wanted_by(2 * sign), origin, count),
        )

    def pick(h, chosen):
        for d in range(2):
            if h == 0:
                step2[d]["scales"].wait_recv()
                for s in range(3):
                    picked_s[d][s] = two_s[d][chosen[d][s]]
                step3[d]["scales"] = send(picked_s[d], three_s[d], d)
            for u in range(count):
                step2[d][u, h].wait_recv()
            for s in range(3):
                picked[d][h][s] = two[d][h][chosen[d][s]]

    def send3(s, h, chosen):
        if s == 2:
            pick(h, chosen)
        for d in range(2):
            step3[d][s, h] = send(picked[d][h].at[s], three[d][h].at[s], d)

    def send4(h):
        for d in range(2):
            if h == 0:
                step3[d]["scales"].wait_recv()
                step4[d]["scales"] = send(three_s[d].at[2], four_s[d].at[0], d)
            step3[d][2, h].wait_recv()
            step4[d][h] = send(three[d][h].at[2], four[d][h].at[0], d)

    each = range(heads)
    def announce(j):
        for d in range(2):
            pl.semaphore_signal(ready.at[d, j], inc=1, **to(ways[d]))

    def hear(j):
        for d in range(2):
            pl.semaphore_wait(ready.at[d, j], 1)

    lanes = ids.shape[1]
    spot = lax.broadcasted_iota(jnp.int32, ids.shape, 0) * lanes
    spot = spot + lax.broadcasted_iota(jnp.int32, ids.shape, 1)
    own = jnp.zeros(ids.shape, jnp.int32)
    for u in range(count):
        start = (within * count + u) * heads
        own = jnp.where((spot >= start) & (spot < start + heads), tokens[u], own)
        own = jnp.where(spot == 2 * lanes + within * count + u, parents[u], own)
    ids[...] = own
    every = range(count)
    announce(0)
    first = [send_to(ids, near.at[k], p) for k, p in enumerate(row_peers)]
    fetch.wait()
    code(0)
    for u in every:
        send1(u, 0)
    hear(0)
    announce(1)
    for h in each[1:]:
        code(h)
    for c in first:
        c.wait_recv()
    total = ids[...]
    for k in range(len(row_peers)):
        total = total + near[k]
    tile[0] = total
    first = [send_to(tile.at[0], side.at[k], p) for k, p in enumerate(col_peers)]
    hear(1)
    announce(2)
    for c in first:
        c.wait_recv()
    for k in range(len(col_peers)):
        total = total + side[k]
    tile[1] = total
    table[0] = total
    hear(2)
    first = [send_to(tile.at[1], table.at[k + 1], p) for k, p in enumerate(beam_peers)]
    for d in range(2):
        step1[d]["scales"] = send(qs, one_s[d], d)
    for h in each[1:-1]:
        for u in every:
            send1(u, h)
    for c in first:
        c.wait_recv()
    to_scalars = pltpu.make_async_copy(table, wants, copied)
    to_scalars.start()
    look_up()
    to_scalars.wait()
    opposite, straight = [], []
    for d in range(2):
        opposite.append(send_to(looked.at[across, halves[d]], opposite_half[d], col_ways[d]))
    for d in range(2):
        straight.append(
            send_to(
                looked.at[cols[d], halves[1 - d]], from_cols[d].at[halves[1 - d]], col_ways[d]
            )
        )
    for d in range(2):
        step1[d]["scales"].wait_recv()
        step2[d]["scales"] = send(one_s[d], two_s[d], d)
    for u in every:
        send1(u, heads - 1)
    for u in every:
        send2(u, 0)
    todo = [functools.partial(send2, u, h) for h in each[1:] for u in every]
    chosen = [choice(d) for d in range(2)]
    for h in each:
        todo.append(functools.partial(send3, 2, h, chosen))
        if h > 0:
            todo.append(functools.partial(send4, h - 1))
        todo.append(functools.partial(send3, 0, h, chosen))
        if h == heads - 1:
            todo.append(functools.partial(send4, h))
        todo.append(functools.partial(send3, 1, h, chosen))
    for d in range(2):
        opposite[d].wait()
        part = part_sum[d]
        add(part, opposite_half[d], looked.at[cols[d], halves[d]])
        straight.append(send_to(part, from_cols[d].at[halves[d]], col_ways[d]))
    for unit in todo[:count]:
        unit()
    for c in straight:
        c.wait_recv()
    add(col_sum, looked.at[col], from_cols[0], from_cols[1])

    swaps = [
        send_to(
            col_sum.at[pl.ds((1 - parity + 2 * i) * BEAMS, BEAMS)],
            from_pair[i], partner,
        )
        for i in range(2)
    ]
    for unit in todo[count : 2 * count]:
        unit()
    todo = todo[2 * count :]
    for c in swaps:
        c.wait_recv()

    def pair(k, _):
        for i in range(2):
            pair_sum[i * BEAMS + k] = col_sum[(parity + 2 * i) * BEAMS + k] + from_pair[i][k]
        return 0

    lax.fori_loop(0, BEAMS, pair, 0)
    reach = (blocks // 4, blocks // 4 - 1)
    passed = [[] for _ in range(2)]

    def block(distance):
        z = (my_beam * rows + row + 2 * blocks + 2 * distance) % blocks
        return (z % rows) // 2 * BEAMS + (my_beam + BEAMS - z // rows) % BEAMS

    def pass_on():
        for d in range(2):
            k = len(passed[d])
            if k == reach[d]:
                continue
            at_block = block(reach[d] - k if d == 0 else k - reach[d])
            if k == 0:
                src = pair_sum.at[at_block]
            else:
                passed[d][k - 1].wait_recv()
                hops[d][k] = pair_sum[at_block] + from_row[d][k - 1]
                src = hops[d].at[k]
            passed[d].append(send_to(src, from_row[d].at[k], row_ways[d]))

    pass_on()
    for i, unit in enumerate(todo):
        unit()
        while len(passed[0]) < min(reach[0], 1 + (i + 1) * reach[0] // len(todo)):
            pass_on()
    for d in range(2):
        passed[d][-1].wait_recv()
    entries[...] = (
        pair_sum[block(0)] + from_row[0][reach[0] - 1] + from_row[1][reach[1] - 1]
    ).astype(jnp.float32)
    for d in range(2):
        step4[d]["scales"].wait_recv()
    mine = wanted_by(0)
    offsets = [(my_beam + BEAMS - mine(u)) % BEAMS for u in every]
    third = [[jnp.where(lowest(mine, beam(b), count) == u, 0, 1) for b in (-3, 3)] for u in every]
    across_first = lowest(mine, beam(4), count)

    def take(x, when, code, scale):
        return jnp.where(when, code.astype(jnp.int32).astype(jnp.float32) * scale, x)

    outs = [[] for _ in every]
    for h in each:
        for d in range(2):
            step3[d][0, h].wait_recv()
            step3[d][1, h].wait_recv()
            step4[d][h].wait_recv()
        at_h = slice(h, h + 1)
        for u in every:
            x = states[u, h]
            offset = offsets[u]
            middle = across_first == u
            for d in range(2):
                t = third[u][d]
                x = take(x, offset == (1, BEAMS - 1)[d], one[d][u, h], one_s[d][u, at_h, :])
                x = take(x, offset == (2, BEAMS - 2)[d], two[d][h][u], two_s[d][u, at_h, :])
                x = take(x, offset == (3, BEAMS - 3)[d], three[d][h][t], three_s[d][t, at_h, :])
                x = take(
                    x, (offset == 4) & (middle if d == 0 else jnp.logical_not(middle)),
                    four[d][h][0], four_s[d][0, at_h, :],
                )
            line = u * heads + h
            state, out = advance(x, lambda k: entries[line : line + 1, k], gain[at_h, :])
            new_states[u, h] = state
            outs[u].append(out)
    for u in every:
        readout[u] = jnp.concatenate(outs[u], axis=0).astype(jnp.bfloat16)
    for c in copies:
        if id(c) not in set(map(id, opposite)):
            c.wait_send()


def step(tokens, parents, states, rows_of_tokens, gain):
    count, heads, size, _ = states.shape
    blocks = lax.axis_size("beam") // ROW
    rows = blocks // BEAMS
    height, width = count * heads, rows_of_tokens.shape[1]
    sends = 2 * heads * (2 * count + 4) + 2 * 4 + 6 + 2 + blocks // 2 - 1 + (rows - 1) + (ROW - 1) + BEAMS - 1
    whole = pl.BlockSpec(memory_space=pltpu.VMEM)
    kept = [count, count, 3, 3, 1, 1, 3, 3]
    parts = [blocks // 2] * 2 + [blocks] * 2 + [blocks // 2] * 2 + [blocks // 4] * 4
    parts += [BEAMS] * 2 + [2 * BEAMS, blocks]
    kind = rows_of_tokens.dtype
    codes, floats, block, ids = jnp.int16, jnp.float32, (height, width), (8, 128)
    scalars = pl.BlockSpec(memory_space=pltpu.SMEM)
    return pl.pallas_call(
        functools.partial(step_kernel, count),
        out_shape=(
            jax.ShapeDtypeStruct((count, heads, size), jnp.bfloat16),
            jax.ShapeDtypeStruct(states.shape, floats),
        ),
        in_specs=[scalars, scalars, pl.BlockSpec(memory_space=pltpu.HBM), whole, whole],
        out_specs=(whole, whole),
        scratch_shapes=[
            *(pltpu.VMEM((k, size, size), codes) for k in kept for _ in range(heads)),
            *(pltpu.VMEM((k, heads, size), floats) for k in kept),
            *(pltpu.VMEM((count, heads, size, size), codes) for _ in range(2)),
            *(pltpu.VMEM((count, heads, size), floats) for _ in range(2)),
            *(pltpu.VMEM((k, *block), kind) for k in parts),
            pltpu.VMEM(block, floats),
            pltpu.VMEM((ROW, blocks, *block), kind),
            pltpu.VMEM(states.shape, floats),
            pltpu.VMEM(states.shape, codes),
            pltpu.VMEM((count, heads, size), floats),
            pltpu.VMEM(ids, jnp.int32),
            pltpu.VMEM((rows - 1, *ids), jnp.int32),
            pltpu.VMEM((ROW - 1, *ids), jnp.int32),
            pltpu.VMEM((2, *ids), jnp.int32),
            pltpu.VMEM((BEAMS, *ids), jnp.int32),
            pltpu.SMEM((BEAMS, *ids), jnp.int32),
            pltpu.SemaphoreType.DMA,
            pltpu.SemaphoreType.DMA,
            pltpu.SemaphoreType.REGULAR((2, BEAMS // 2 - 1)),
            pltpu.SemaphoreType.DMA((sends,)),
            pltpu.SemaphoreType.DMA((sends,)),
        ],
        compiler_params=pltpu.CompilerParams(
            collective_id=0, has_side_effects=True, vmem_limit_bytes=48 << 20
        ),
    )(tokens, parents, states, rows_of_tokens, gain)


def local(states, parent_beam, next_token, proj_table, gate_table, gain):
    heads, size = states.shape[1:3]
    vocab_rows = proj_table.shape[0]
    padded = jnp.concatenate(
        [
            proj_table.transpose(1, 0, 2),
            gate_table.transpose(2, 0, 1),
            jnp.zeros((heads, vocab_rows, size - 3), proj_table.dtype),
        ],
        axis=2,
    ).reshape(heads * vocab_rows, 6 * size)
    return step(next_token, parent_beam, states, padded, gain)


def solution(mesh):
    return jax.shard_map(
        local,
        mesh=mesh,
        in_specs=(
            P(("groups", "beam"), "mp", None, None),
            P(("groups", "beam")),
            P(("groups", "beam")),
            P("beam", "mp", None),
            P("beam", None, "mp"),
            P("mp", None),
        ),
        out_specs=(P(("groups", "beam"), "mp", None), P(("groups", "beam"), "mp", None, None)),
        check_vma=False,
    )
```
